128 devices in a mesh: section: 16 (over x, y_lo, core), tensor: 8 (over y_hi, z).
Axes of the slice: x: 4, y: 4 (y_hi: 2, y_lo: 2; y = y_hi * 2 + y_lo), z: 4, core: 2. Of those that a mesh axis runs over, the one named last changes fastest.
Arguments:
- arriving: bfloat16 [16, 1024, 16384], P('section', 'tensor'), may hold values from -6 to 6
- kept_input: bfloat16 [16, 1024, 16384], P('section', 'tensor'), may hold values from -6 to 6
- returning: bfloat16 [16, 1024, 16384], P('section', 'tensor'), may hold values from -6 to 6
- norm_gain: bfloat16 [16, 16384], P('section'), may hold values from 0.25 to 1.75
- key_weight: bfloat16 [16, 16384, 1024], P('section', 'tensor'), may hold values from -0.0625 to 0.0625
- value_weight: bfloat16 [16, 16384, 1024], P('section', 'tensor'), may hold values from -0.0625 to 0.0625
- key_down: bfloat16 [16, 16384, 16], P('section', 'tensor'), may hold values from -0.046875 to 0.046875
- value_down: bfloat16 [16, 16384, 16], P('section', 'tensor'), may hold values from -0.046875 to 0.046875
- key_up: bfloat16 [16, 16, 1024], P('section', None, 'tensor'), may hold values from -1.5 to 1.5
- value_up: bfloat16 [16, 16, 1024], P('section', None, 'tensor'), may hold values from -1.5 to 1.5
- key_cot: bfloat16 [16, 1024, 1024], P('section', None, 'tensor'), may hold values from -6 to 6
- value_cot: bfloat16 [16, 1024, 1024], P('section', None, 'tensor'), may hold values from -6 to 6
Outputs:
- keys: bfloat16 [16, 1024, 1024], P('section', None, 'tensor')
- values: bfloat16 [16, 1024, 1024], P('section', None, 'tensor')
- input_grad: bfloat16 [16, 1024, 16384], P('section', 'tensor')
- key_down_grad: float32 [16, 16384, 16], P('section', 'tensor')
- value_down_grad: float32 [16, 16384, 16], P('section', 'tensor')
- key_up_grad: float32 [16, 16, 1024], P('section', None, 'tensor')
- value_up_grad: float32 [16, 16, 1024], P('section', None, 'tensor')
The draws below stay inside these ranges and needn't reach their ends.
All inputs are finite; a program needn't handle non-finite values.
Results may differ from the reference program's by a relative error of at most 0.014.
Values may be sent and summed in bfloat16 or wider, within the bound.
A program may use at most 192 MiB of HBM per device.

```python
import jax
import jax.numpy as jnp
from jax import lax

D = 16384
RANK = 16
TOKENS = 1024
KVW = 1024
LAYERS = 16


def with_spikes(values, stream_key, source, target, blocks, factor):
    def block_of(position):
        return (jnp.arange(values.shape[position]) // (values.shape[position] // blocks)).reshape((-1,) + (1,) * (values.ndim - 1 - position))

    one_side = jax.random.permutation(stream_key, blocks)[block_of(target)]
    other_side = (block_of(target) + blocks // 2) % blocks
    return jnp.where((block_of(source) == one_side) | (block_of(source) == other_side), factor * values, values)


def block_scale(stream_key, dims, cuts, low, high):
    level = 1.0
    for position, shards_of in cuts:
        draws = jax.random.uniform(jax.random.fold_in(jax.random.fold_in(stream_key, 6), position), (shards_of,), jnp.float32, low / len(cuts), high / len(cuts))
        level = level * jnp.repeat(jnp.exp(draws), dims[position] // shards_of).reshape((-1,) + (1,) * (len(dims) - 1 - position))
    return level


def bell_draw(key, extent, scale, reach, shards=(), held_as=jnp.bfloat16):
    factor_of = block_scale(key, extent, shards, -0.22, 0.18) if shards else 1.0
    result = jax.random.normal(key, extent, jnp.float32) * scale * factor_of
    return jnp.minimum(jnp.maximum(result, -reach), reach).astype(held_as)


def noise_with(stream_key, extent, spread, bound, pieces, heavy, dtype=jnp.bfloat16):
    entries = spread * jax.random.normal(stream_key, extent, jnp.float32)
    if pieces:
        entries = entries * block_scale(stream_key, extent, pieces, -0.22, 0.18)
    return jnp.clip(with_spikes(entries, jax.random.fold_in(stream_key, 3), *heavy), -bound, bound).astype(dtype)


def setup_inputs(seed: int = 0) -> dict:
    key_of = jax.random.split(jax.random.key(seed), 13)
    return {
        "arriving": bell_draw(key_of[0], (LAYERS, TOKENS, D), 1.0, 6.0, ((0, 16), (1, 8))),
        "kept_input": bell_draw(key_of[1], (LAYERS, TOKENS, D), 1.0, 6.0, ((0, 16), (1, 8))),
        "returning": bell_draw(key_of[2], (LAYERS, TOKENS, D), 1.0, 6.0, ((0, 16), (1, 8))),
        "norm_gain": jnp.clip(1.0 + 0.15 * jax.random.normal(key_of[3], (LAYERS, D), jnp.float32), 0.25, 1.75).astype(jnp.bfloat16),
        "key_weight": noise_with(key_of[4], (LAYERS, D, KVW), D ** -0.5, 0.0625, ((0, 16), (1, 8)), (1, 2, 8, 2.0)),
        "value_weight": noise_with(key_of[5], (LAYERS, D, KVW), D ** -0.5, 0.0625, ((0, 16), (1, 8)), (1, 2, 8, 2.0)),
        "key_down": bell_draw(key_of[6], (LAYERS, D, RANK), D ** -0.5, 0.046875, ((0, 16), (1, 8))),
        "value_down": bell_draw(key_of[7], (LAYERS, D, RANK), D ** -0.5, 0.046875, ((0, 16), (1, 8))),
        "key_up": bell_draw(key_of[8], (LAYERS, RANK, KVW), RANK ** -0.5, 1.5, ((0, 16), (2, 8))),
        "value_up": bell_draw(key_of[9], (LAYERS, RANK, KVW), RANK ** -0.5, 1.5, ((0, 16), (2, 8))),
        "key_cot": bell_draw(key_of[10], (LAYERS, TOKENS, KVW), 1.0, 6.0, ((0, 16), (2, 8))),
        "value_cot": bell_draw(key_of[11], (LAYERS, TOKENS, KVW), 1.0, 6.0, ((0, 16), (2, 8))),
    }


epsilon = 1e-05
adapter_scale = 2.0

def normalize(hidden, gain):
    values = hidden.astype(jnp.float32)
    inverse = lax.rsqrt(lax.optimization_barrier(jnp.mean(values * values, axis=-1, keepdims=True)) + epsilon)
    return (inverse, (values * inverse * gain.astype(jnp.float32)).astype(jnp.bfloat16))

def precise_product(left, right):
    return jnp.dot(left, right, precision=lax.Precision.HIGHEST, preferred_element_type=jnp.float32)

def mixed_product(left, right):
    return jnp.dot(left.astype(jnp.float32), right.astype(jnp.float32), preferred_element_type=jnp.float32)

def one_layer(blocks):
    incoming, kept, back, gain, key_matrix, value_matrix, key_down_matrix, value_down_matrix, key_up_matrix, value_up_matrix, key_cotangent, value_cotangent = blocks
    _, normed_input = normalize(incoming, gain)
    key_middle = mixed_product(normed_input, key_down_matrix)
    value_middle = mixed_product(normed_input, value_down_matrix)
    keys = (mixed_product(normed_input, key_matrix) + adapter_scale * precise_product(key_middle, key_up_matrix.astype(jnp.float32))).astype(jnp.bfloat16)
    values = (mixed_product(normed_input, value_matrix) + adapter_scale * precise_product(value_middle, value_up_matrix.astype(jnp.float32))).astype(jnp.bfloat16)
    adapted_key = mixed_product(key_cotangent, key_up_matrix.T)
    adapted_value = mixed_product(value_cotangent, value_up_matrix.T)
    branch_output = mixed_product(key_cotangent, key_matrix.T) + mixed_product(value_cotangent, value_matrix.T)
    branch_output = branch_output + adapter_scale * (precise_product(adapted_key, key_down_matrix.T.astype(jnp.float32)) + precise_product(adapted_value, value_down_matrix.T.astype(jnp.float32)))
    branch_output = lax.optimization_barrier(branch_output.astype(jnp.bfloat16)).astype(jnp.float32)
    inverse, kept_normed = normalize(kept, gain)
    kept_values = kept.astype(jnp.float32)
    scaled = gain.astype(jnp.float32) * branch_output
    inner = lax.optimization_barrier(jnp.mean(kept_values * scaled, axis=-1, keepdims=True))
    input_grad = (back.astype(jnp.float32) + inverse * scaled - kept_values * inverse * inverse * inverse * inner).astype(jnp.bfloat16)
    saved_wide_input = kept_normed.astype(jnp.float32)
    key_down_gradient = adapter_scale * precise_product(saved_wide_input.T, adapted_key)
    value_down_gradient = adapter_scale * precise_product(saved_wide_input.T, adapted_value)
    key_middle_rows = mixed_product(kept_normed, key_down_matrix)
    value_middle_rows = mixed_product(kept_normed, value_down_matrix)
    key_up_gradient = adapter_scale * precise_product(key_middle_rows.T, key_cotangent.astype(jnp.float32))
    value_up_gradient = adapter_scale * precise_product(value_middle_rows.T, value_cotangent.astype(jnp.float32))
    return (keys, values, input_grad, key_down_gradient, value_down_gradient, key_up_gradient, value_up_gradient)

def reference(arriving, kept_input, returning, norm_gain, key_weight, value_weight, key_down, value_down, key_up, value_up, key_cot, value_cot):
    incoming = jnp.roll(arriving, 1, axis=0)
    back = jnp.roll(returning, -1, axis=0)
    layer_count = arriving.shape[0]
    collected = []
    for layer in range(layer_count):
        blocks = (incoming[layer], kept_input[layer], back[layer], norm_gain[layer], key_weight[layer], value_weight[layer], key_down[layer], value_down[layer], key_up[layer], value_up[layer], key_cot[layer], value_cot[layer])
        collected.append(one_layer(blocks))
    stacked = [jnp.stack([item[index] for item in collected], axis=0) for index in range(7)]
    return (stacked[0], stacked[1], stacked[2], stacked[3], stacked[4], stacked[5], stacked[6])
```

```python
import functools

import jax
import jax.numpy as jnp
from jax import lax
from jax.experimental import pallas as pl
from jax.experimental.pallas import tpu as pltpu
from jax.sharding import PartitionSpec as P

EPS = 1e-05
SCALE = 2.0
F32 = jnp.float32
BF16 = jnp.bfloat16
MESH = pl.DeviceIdType.MESH

UPK, UPV, DNK, DNV, COTK, COTV, XIN, INV, RET, BRA, GRD, MID = range(12)
KINDS = 12


def dot(a, b, ca, cb):
    return lax.dot_general(a, b, (((ca,), (cb,)), ((), ())), preferred_element_type=F32)


def kernel(
    S, T, G,
    arr, kept, ret, gain, wk, wv, dkt, dvt, uk, uv, ck, cv,
    keys, vals, igrad, gkt, gvt, guk, guv,
    wb, cf, xin, kb, back, bro, bri, yo, yi, dnf, gdo, gdi, upf, inv_o, inv_i, mid_o, mid_i, inv_b,
    ss, rs, yss, yrs, ls, ols,
):
    sec = lax.axis_index("section")
    t = lax.axis_index("tensor")
    R = arr.shape[0]
    DS = wk.shape[0]
    H = ck.shape[1]
    KV = wk.shape[1]
    RK = uk.shape[0]
    D = T * DS
    nxt = lax.rem(sec + 1, S)
    prv = lax.rem(sec + S - 1, S)

    def to(i):
        return lax.rem(t + i, T)

    def frm(i):
        return lax.rem(t + T - i, T)

    def blk(i, size):
        return pl.ds(pl.multiple_of(i * size, size), size)

    def send(src, dst, kind, i, device):
        return pltpu.make_async_remote_copy(
            src_ref=src, dst_ref=dst, send_sem=ss.at[kind, i], recv_sem=rs.at[kind, i],
            device_id=device, device_id_type=MESH,
        )

    bar = pltpu.get_barrier_semaphore()
    for i in range(1, T):
        pl.semaphore_signal(bar, inc=1, device_id=(sec, to(i)), device_id_type=MESH)
    for i in range(T):
        pl.semaphore_signal(bar, inc=1, device_id=(nxt, to(i)), device_id_type=MESH)
        pl.semaphore_signal(bar, inc=1, device_id=(prv, to(i)), device_id_type=MESH)
    pl.semaphore_wait(bar, 3 * T - 1)

    def small(i):
        dev = (sec, to(i))
        return (
            send(uk, upf.at[pl.ds(0, RK), blk(t, H)], UPK, i, dev),
            send(uv, upf.at[pl.ds(RK, RK), pl.ds(pl.multiple_of(KV + t * H, H), H)], UPV, i, dev),
            send(dkt, dnf.at[pl.ds(0, RK), blk(t, DS)], DNK, i, dev),
            send(dvt, dnf.at[pl.ds(RK, RK), blk(t, DS)], DNV, i, dev),
        )

    def cots(i):
        dev = (sec, to(i))
        return (
            send(ck, cf.at[:, blk(t, H)], COTK, i, dev),
            send(cv, cf.at[:, pl.ds(pl.multiple_of(KV + t * H, H), H)], COTV, i, dev),
        )

    def xs(i):
        return send(arr.at[:, blk(to(i), DS)], xin.at[blk(t, R), :], XIN, i, (nxt, to(i)))

    def invs(i):
        return send(inv_o, inv_i.at[i], INV, i, (nxt, to(i)))

    def rets():
        return send(ret, back, RET, 0, (prv, t))

    def bras(i):
        return send(bro.at[to(i)], bri.at[i], BRA, i, (sec, to(i)))

    def grds(i):
        return send(gdo.at[to(i)], gdi.at[i], GRD, i, (sec, to(i)))

    def mids(i):
        return send(mid_o, mid_i.at[i], MID, i, (sec, to(i)))

    RG = R * T // G

    def ysend(g, i):
        p = to(i)
        out = []
        for v in range(2):
            out.append(pltpu.make_async_remote_copy(
                src_ref=yo.at[pl.ds(g * RG, RG), pl.ds(pl.multiple_of(v * KV + p * H, H), H)],
                dst_ref=yi.at[i, pl.ds(g * RG, RG), pl.ds(v * H, H)],
                send_sem=yss.at[2 * g + v, i], recv_sem=yrs.at[2 * g + v, i],
                device_id=(sec, p), device_id_type=MESH,
            ))
        return out

    for i in range(1, T):
        for c in small(i):
            c.start()
    for i in range(1, T):
        for c in cots(i):
            c.start()
    for i in range(T):
        xs(i).start()
    rets().start()

    loc = [
        pltpu.make_async_copy(wk, wb.at[:, pl.ds(0, KV)], ls.at[0]),
        pltpu.make_async_copy(wv, wb.at[:, pl.ds(KV, KV)], ls.at[1]),
        pltpu.make_async_copy(uk, upf.at[pl.ds(0, RK), blk(t, H)], ls.at[2]),
        pltpu.make_async_copy(uv, upf.at[pl.ds(RK, RK), pl.ds(pl.multiple_of(KV + t * H, H), H)], ls.at[3]),
        pltpu.make_async_copy(dkt, dnf.at[pl.ds(0, RK), blk(t, DS)], ls.at[4]),
        pltpu.make_async_copy(dvt, dnf.at[pl.ds(RK, RK), blk(t, DS)], ls.at[5]),
        pltpu.make_async_copy(ck, cf.at[:, blk(t, H)], ls.at[6]),
        pltpu.make_async_copy(cv, cf.at[:, pl.ds(pl.multiple_of(KV + t * H, H), H)], ls.at[7]),
        pltpu.make_async_copy(kept, kb, ls.at[8]),
    ]
    arrs = [pltpu.make_async_copy(arr.at[:, pl.ds(j * DS, DS)], bro.at[j], ls.at[9 + j]) for j in range(T)]
    for c in arrs:
        c.start()
    for c in loc:
        c.start()
    upf[pl.ds(0, RK), pl.ds(KV, KV)] = jnp.zeros((RK, KV), BF16)
    upf[pl.ds(RK, RK), pl.ds(0, KV)] = jnp.zeros((RK, KV), BF16)

    for c in arrs:
        c.wait()

    def sq_a(j, acc):
        v = bro[j].astype(F32)
        return acc + jnp.sum(v * v, axis=-1, keepdims=True)

    total = lax.fori_loop(0, T, sq_a, jnp.zeros((R, 1), F32))
    inverse = lax.rsqrt(total / D + EPS)
    inv_o[...] = jnp.broadcast_to(inverse, (R, R)).T[0:8, :]
    for i in range(T):
        invs(i).start()

    for c in loc:
        c.wait()

    def sq_b(j, acc):
        v = kb[:, blk(j, DS)].astype(F32)
        return acc + jnp.sum(v * v, axis=-1, keepdims=True)

    total = lax.fori_loop(0, T, sq_b, jnp.zeros((R, 1), F32))
    inv_b[...] = jnp.broadcast_to(lax.rsqrt(total / D + EPS), (R, R))

    def wait_small(i):
        dev = (sec, to(i))
        r = frm(i)
        send(uk, upf.at[pl.ds(0, RK), blk(r, H)], UPK, i, dev).wait_recv()
        send(uv, upf.at[pl.ds(RK, RK), pl.ds(pl.multiple_of(KV + r * H, H), H)], UPV, i, dev).wait_recv()
        send(dkt, dnf.at[pl.ds(0, RK), blk(r, DS)], DNK, i, dev).wait_recv()
        send(dvt, dnf.at[pl.ds(RK, RK), blk(r, DS)], DNV, i, dev).wait_recv()

    for i in range(1, T):
        wait_small(i)
    WT = 256

    def weff(j, _):
        down = dnf[:, pl.ds(pl.multiple_of(t * DS + j * WT, WT), WT)]
        low = dot(down, upf[...], 0, 0)
        rows = blk(j, WT)
        wb[rows, :] = (wb[rows, :].astype(F32) + SCALE * low).astype(BF16)
        return 0

    lax.fori_loop(0, DS // WT, weff, 0)

    for i in range(1, T):
        r = frm(i)
        dev = (sec, to(i))
        send(ck, cf.at[:, blk(r, H)], COTK, i, dev).wait_recv()
        send(cv, cf.at[:, pl.ds(pl.multiple_of(KV + r * H, H), H)], COTV, i, dev).wait_recv()
    NT = 512

    def branch(p, store):
        c = cf[blk(p, R), :]
        for n in range(DS // NT):
            store(n, dot(c, wb[pl.ds(n * NT, NT), :], 1, 1).astype(BF16))

    def branch_to(i, _):
        p = to(i)

        def store(n, v):
            bro[p, :, pl.ds(n * NT, NT)] = v

        branch(p, store)
        bras(i).start()
        return 0

    lax.fori_loop(1, T, branch_to, 0)

    def store_own(n, v):
        bri[0, :, pl.ds(n * NT, NT)] = v

    branch(t, store_own)

    adapt = (SCALE * dot(upf[...], cf[blk(t, R), :], 1, 1)).astype(BF16)

    def kept_block(i, mid):
        p = to(i)
        cols = blk(p, DS)
        normed = (kb[:, cols].astype(F32) * inv_b[:, 0:1] * gain[:, cols].astype(F32)).astype(BF16)
        gdo[p] = dot(adapt, normed, 1, 0).astype(BF16)

        @pl.when(i > 0)
        def _():
            grds(i).start()

        return mid + dot(dnf[:, cols], normed, 1, 1)

    mid = lax.fori_loop(0, T, kept_block, jnp.zeros((2 * RK, R), F32))
    mid_o[...] = mid.astype(BF16)
    for i in range(1, T):
        mids(i).start()

    def forward(i, _):
        r = frm(i)
        send(arr.at[:, blk(to(i), DS)], xin.at[blk(r, R), :], XIN, i, (nxt, to(i))).wait_recv()
        invs(i).wait_recv()
        inv = jnp.broadcast_to(inv_i[i, 0:1, :], (R, R)).T
        normed = (
            xin[blk(r, R), :].astype(F32) * inv[:, 0:1] * gain[:, blk(t, DS)].astype(F32)
        ).astype(BF16)
        rows = blk(i, R)
        for n in range(2 * KV // NT):
            yo[rows, pl.ds(n * NT, NT)] = dot(normed, wb[:, pl.ds(n * NT, NT)], 1, 0).astype(BF16)
        return 0

    for g in range(G):
        lax.fori_loop(g * (T // G), (g + 1) * (T // G), forward, 0)
        for i in range(1, T):
            for c in ysend(g, i):
                c.start()

    for i in range(1, T):
        grds(i).wait_recv()
        mids(i).wait_recv()
    g = gdo[t].astype(F32)
    for i in range(1, T):
        g = g + gdi[i].astype(F32)
    gkt[...] = g[0:RK]
    gvt[...] = g[RK : 2 * RK]

    def up_grad(i, acc):
        r = frm(i)
        m = mid_i[i]
        rows = blk(r, R)
        k = dot(m[0:RK], cf[rows, blk(t, H)], 1, 0)
        v = dot(m[RK : 2 * RK], cf[rows, pl.ds(pl.multiple_of(KV + t * H, H), H)], 1, 0)
        return acc[0] + k, acc[1] + v

    mid_i[0] = mid_o[...]
    k, v = lax.fori_loop(0, T, up_grad, (jnp.zeros((RK, H), F32), jnp.zeros((RK, H), F32)))
    guk[...] = SCALE * k
    guv[...] = SCALE * v

    for i in range(1, T):
        bras(i).wait_recv()

    def inner_block(i, acc):
        cols = blk(frm(i), DS)
        scaled = gain[:, cols].astype(F32) * bri[i].astype(F32)
        return acc + jnp.sum(kb[:, cols].astype(F32) * scaled, axis=-1, keepdims=True)

    inner = lax.fori_loop(0, T, inner_block, jnp.zeros((R, 1), F32)) / D
    send(ret, back, RET, 0, (prv, t)).wait_recv()
    inverse = inv_b[:, 0:1]
    factor = inverse * inverse * inverse * inner

    def final_block(i, _):
        cols = blk(frm(i), DS)
        scaled = gain[:, cols].astype(F32) * bri[i].astype(F32)
        back[:, cols] = (
            back[:, cols].astype(F32) + inverse * scaled - kb[:, cols].astype(F32) * factor
        ).astype(BF16)
        pltpu.make_async_copy(back.at[:, cols], igrad.at[:, cols], ols.at[i]).start()
        return 0

    lax.fori_loop(0, T, final_block, 0)

    for g in range(G):
        for i in range(1, T):
            for c in ysend(g, i):
                c.wait_recv()

    def total_block(b, _):
        own = blk(lax.rem(t + T - b, T), R)
        k = yo[own, blk(t, H)].astype(F32)
        v = yo[own, pl.ds(pl.multiple_of(KV + t * H, H), H)].astype(F32)
        for i in range(1, T):
            rows = blk(lax.rem(t + 2 * T - i - b, T), R)
            k = k + yi[i, rows, pl.ds(0, H)].astype(F32)
            v = v + yi[i, rows, pl.ds(H, H)].astype(F32)
        keys[blk(b, R), :] = k.astype(BF16)
        vals[blk(b, R), :] = v.astype(BF16)
        return 0

    lax.fori_loop(0, T, total_block, 0)

    for i in range(1, T):
        for c in (*small(i), *cots(i), bras(i), grds(i), mids(i)):
            c.wait_send()
        for g in range(G):
            for c in ysend(g, i):
                c.wait_send()
    for i in range(T):
        xs(i).wait_send()
        invs(i).wait_send()
        cols = blk(frm(i), DS)
        pltpu.make_async_copy(back.at[:, cols], igrad.at[:, cols], ols.at[i]).wait()
    rets().wait_send()


def on_device(S, T, arr, kept, ret, gain, wk, wv, dk, dv, uk, uv, ck, cv):
    G = 2
    _, R, D = arr.shape
    _, DS, KV = wk.shape
    RK, H = uk.shape[1:]
    any_ = pl.BlockSpec(memory_space=pl.ANY)
    vmem = pl.BlockSpec(memory_space=pltpu.VMEM)
    outs = pl.pallas_call(
        functools.partial(kernel, S, T, G),
        out_shape=(
            jax.ShapeDtypeStruct((R * T, H), BF16),
            jax.ShapeDtypeStruct((R * T, H), BF16),
            jax.ShapeDtypeStruct((R, D), BF16),
            jax.ShapeDtypeStruct((RK, DS), F32),
            jax.ShapeDtypeStruct((RK, DS), F32),
            jax.ShapeDtypeStruct((RK, H), F32),
            jax.ShapeDtypeStruct((RK, H), F32),
        ),
        in_specs=[any_, any_, any_, vmem] + [any_] * 8,
        out_specs=(vmem, vmem, any_, vmem, vmem, vmem, vmem),
        scratch_shapes=[
            pltpu.VMEM((DS, 2 * KV), BF16),
            pltpu.VMEM((R * T, 2 * KV), BF16),
            pltpu.VMEM((R * T, DS), BF16),
            pltpu.VMEM((R, D), BF16),
            pltpu.VMEM((R, D), BF16),
            pltpu.VMEM((T, R, DS), BF16),
            pltpu.VMEM((T, R, DS), BF16),
            pltpu.VMEM((R * T, 2 * KV), BF16),
            pltpu.VMEM((T, R * T, 2 * H), BF16),
            pltpu.VMEM((2 * RK, D), BF16),
            pltpu.VMEM((T, 2 * RK, DS), BF16),
            pltpu.VMEM((T, 2 * RK, DS), BF16),
            pltpu.VMEM((2 * RK, 2 * KV), BF16),
            pltpu.VMEM((8, R), F32),
            pltpu.VMEM((T, 8, R), F32),
            pltpu.VMEM((2 * RK, R), BF16),
            pltpu.VMEM((T, 2 * RK, R), BF16),
            pltpu.VMEM((R, R), F32),
            pltpu.SemaphoreType.DMA((KINDS, T)),
            pltpu.SemaphoreType.DMA((KINDS, T)),
            pltpu.SemaphoreType.DMA((2 * G, T)),
            pltpu.SemaphoreType.DMA((2 * G, T)),
            pltpu.SemaphoreType.DMA((9 + T,)),
            pltpu.SemaphoreType.DMA((T,)),
        ],
        compiler_params=pltpu.CompilerParams(
            collective_id=0, has_side_effects=True, vmem_limit_bytes=62 * 2**20
        ),
    )(
        arr[0], kept[0], ret[0], gain, wk[0], wv[0], dk[0].T, dv[0].T, uk[0], uv[0], ck[0], cv[0]
    )
    keys, vals, igrad, gkt, gvt, guk, guv = outs
    return keys[None], vals[None], igrad[None], gkt.T[None], gvt.T[None], guk[None], guv[None]


def solution(mesh):
    S, T = mesh.shape["section"], mesh.shape["tensor"]
    return jax.shard_map(
        functools.partial(on_device, S, T),
        mesh=mesh,
        in_specs=(
            P("section", "tensor", None),
            P("section", "tensor", None),
            P("section", "tensor", None),
            P("section", None),
            P("section", "tensor", None),
            P("section", "tensor", None),
            P("section", "tensor", None),
            P("section", "tensor", None),
            P("section", None, "tensor"),
            P("section", None, "tensor"),
            P("section", None, "tensor"),
            P("section", None, "tensor"),
        ),
        out_specs=(
            P("section", None, "tensor"),
            P("section", None, "tensor"),
            P("section", "tensor", None),
            P("section", "tensor", None),
            P("section", "tensor", None),
            P("section", None, "tensor"),
            P("section", None, "tensor"),
        ),
        check_vma=False,
    )
```

```python
import contextlib
import functools

import jax
import jax.numpy as jnp
from jax import lax
from jax.experimental import pallas as pl
from jax.experimental.pallas import tpu as pltpu
from jax.sharding import PartitionSpec as P

EPS = 1e-05
SCALE = 2.0
F32 = jnp.float32
BF16 = jnp.bfloat16
MESH = pl.DeviceIdType.MESH

UPK, UPV, DNK, DNV, COT, XAT, XIN, INV, RET, BRA, GRD, MID, PAR, TOT = range(14)
KINDS = 14


PROFILE = False


def scope(name):
    return jax.named_scope(name) if PROFILE else contextlib.nullcontext()


def dot(a, b, ca, cb):
    return lax.dot_general(a, b, (((ca,), (cb,)), ((), ())), preferred_element_type=F32)


def kernel(
    S, Y, Z,
    arr, kept, ret, gain, wk, wv, dkt, dvt, uk, uv, ck, cv,
    keys, vals, igrad, gkt, gvt, guk, guv,
    wb, cf, xin, xat, kb, back, bro, bri, yo, yi, yco, yci, yt, ys, yr, dnf, gdo, gdi, upf,
    inv_o, inv_i, mid_o, mid_i, inv_b,
    ss, rs, css, crs, yss, yrs, ls, ols,
):
    sec = lax.axis_index("section")
    t = lax.axis_index("tensor")
    T = Y * Z
    R = arr.shape[0]
    DS = wk.shape[0]
    H = ck.shape[1]
    KV = wk.shape[1]
    RK = uk.shape[0]
    D = T * DS
    nxt = lax.rem(sec + 1, S)
    prv = lax.rem(sec + S - 1, S)
    y = t // Z
    z = lax.rem(t, Z)

    def to(i):
        return lax.rem(y + i // Z, Y) * Z + lax.rem(z + lax.rem(i, Z), Z)

    def frm(i):
        return lax.rem(y + Y - i // Z, Y) * Z + lax.rem(z + Z - lax.rem(i, Z), Z)

    def blk(i, size):
        return pl.ds(pl.multiple_of(i * size, size), size)

    def vblk(i):
        return pl.ds(pl.multiple_of(KV + i * H, H), H)

    def remote(src, dst, ssem, rsem, device):
        return pltpu.make_async_remote_copy(
            src_ref=src, dst_ref=dst, send_sem=ssem, recv_sem=rsem,
            device_id=device, device_id_type=MESH,
        )

    def send(src, dst, kind, i, device):
        return remote(src, dst, ss.at[kind, i], rs.at[kind, i], device)

    def ups(i, r):
        dev = (sec, to(i))
        return (
            send(uk, upf.at[pl.ds(0, RK), blk(r, H)], UPK, i, dev),
            send(uv, upf.at[pl.ds(RK, RK), vblk(r)], UPV, i, dev),
        )

    def downs(i, r):
        dev = (sec, to(i))
        return (
            send(dkt, dnf.at[pl.ds(0, RK), blk(r, DS)], DNK, i, dev),
            send(dvt, dnf.at[pl.ds(RK, RK), blk(r, DS)], DNV, i, dev),
        )

    def cot_part(v, i, q, r, own):
        at, to_at = (blk(q, H), blk(r, H)) if v == 0 else (vblk(q), vblk(r))
        dy, dz = i // Z, i % Z
        if dz == 2:
            dev = (sec, to(1 if v == 0 else Z - 1))
        else:
            dev = (sec, to(dz if dz else dy * Z))
        src = (ck, cv)[v] if own else cf.at[:, at]
        return remote(src, cf.at[:, to_at], css.at[v, i], crs.at[v, i], dev)

    def cots(i, q, r, own=False):
        return [cot_part(v, i, q, r, own) for v in range(2)]

    def xfirst(i, r):
        dy, dz = i // Z, i % Z
        cols = blk(lax.rem(y + dy, Y) * Z + lax.rem(z + dz, Z), DS)
        dst = xin.at[blk(r, R), :] if dz == 0 else xat.at[dy * (Z - 1) + dz - 1]
        return send(arr.at[:, cols], dst, XAT, i, (nxt, to(dy * Z)))

    def xon(i, q, r):
        dy, dz = i // Z, i % Z
        return send(xat.at[dy * (Z - 1) + dz - 1], xin.at[blk(r, R), :], XIN, i, (sec, to(dz)))

    def invs(i):
        return send(inv_o, inv_i.at[i], INV, i, (nxt, to(i)))

    def rets():
        return send(ret, back, RET, 0, (prv, t))

    def bras(i):
        return send(bro.at[to(i)], bri.at[i], BRA, i, (sec, to(i)))

    def grds(i):
        return send(gdo.at[to(i)], gdi.at[i], GRD, i, (sec, to(i)))

    def mids(i):
        return send(mid_o, mid_i.at[i], MID, i, (sec, to(i)))

    RG = R * Z

    def parts(g, k):
        v = k % 2
        dz = (1, Z - 1, Z - 1, 1)[k]
        zz = lax.rem(z + (2 if k < 2 else dz), Z)
        out = []
        for w in range(Y):
            at = pl.multiple_of(v * KV + (w * Z + zz) * H, H)
            n = (g * 4 + k) * Y + w
            out.append(remote(
                yo.at[pl.ds(g * RG, RG), pl.ds(at, H)],
                yi.at[k, pl.ds(g * RG, RG), pl.ds(w * H, H)],
                yss.at[n], yrs.at[n], (sec, to(dz)),
            ))
        return out

    def pairs(g, v, row):
        return send(yco.at[v, blk(row, RG), :], yci.at[v, blk(row, RG), :], PAR, g * 2 + v, (sec, to(1 if v == 0 else Z - 1)))

    def tots(g, dy, row):
        return send(ys.at[dy, blk(row, RG), :], yr.at[dy, blk(row, RG), :], TOT, g * Y + dy, (sec, to(dy * Z)))

    bar = pltpu.get_barrier_semaphore()
    for i in range(1, T):
        pl.semaphore_signal(bar, inc=1, device_id=(sec, to(i)), device_id_type=MESH)
    for i in range(T):
        pl.semaphore_signal(bar, inc=1, device_id=(nxt, to(i)), device_id_type=MESH)
        pl.semaphore_signal(bar, inc=1, device_id=(prv, to(i)), device_id_type=MESH)

    arrs = [pltpu.make_async_copy(arr.at[:, pl.ds(j * DS, DS)], bro.at[j], ls.at[9 + j]) for j in range(T)]
    loc = [
        pltpu.make_async_copy(wk, wb.at[:, pl.ds(0, KV)], ls.at[0]),
        pltpu.make_async_copy(wv, wb.at[:, pl.ds(KV, KV)], ls.at[1]),
        pltpu.make_async_copy(uk, upf.at[pl.ds(0, RK), blk(t, H)], ls.at[2]),
        pltpu.make_async_copy(uv, upf.at[pl.ds(RK, RK), vblk(t)], ls.at[3]),
        pltpu.make_async_copy(dkt, dnf.at[pl.ds(0, RK), blk(t, DS)], ls.at[4]),
        pltpu.make_async_copy(dvt, dnf.at[pl.ds(RK, RK), blk(t, DS)], ls.at[5]),
        pltpu.make_async_copy(ck, cf.at[:, blk(t, H)], ls.at[6]),
        pltpu.make_async_copy(cv, cf.at[:, vblk(t)], ls.at[7]),
        pltpu.make_async_copy(kept, kb, ls.at[8]),
    ]
    for c in arrs:
        c.start()
    for c in loc:
        c.start()
    upf[pl.ds(0, RK), pl.ds(KV, KV)] = jnp.zeros((RK, KV), BF16)
    upf[pl.ds(RK, RK), pl.ds(0, KV)] = jnp.zeros((RK, KV), BF16)

    with scope("barrier"):
        pl.semaphore_wait(bar, 3 * T - 1)

    for i in range(1, T):
        for c in ups(i, t):
            c.start()
    for dy in range(1, Y):
        for c in cots(dy * Z, t, t, True):
            c.start()
    for i in (1, Z - 1):
        for c in cots(i, t, t, True):
            c.start()
    with scope("stats_a"):
        for c in arrs:
            c.wait()

        def sq_a(j, acc):
            v = bro[j].astype(F32)
            return acc + jnp.sum(v * v, axis=-1, keepdims=True)

        total = lax.fori_loop(0, T, sq_a, jnp.zeros((R, 1), F32))
        inverse = lax.rsqrt(total / D + EPS)
        inv_o[...] = jnp.broadcast_to(inverse, (R, R)).T[0:8, :]
        for i in range(T):
            invs(i).start()

    def cot_wait(i):
        for c in cots(i, t, frm(i)):
            c.wait_recv()

    def cot_halves(dy):
        for v in range(2):
            q = frm(dy * Z + (1 if v == 0 else Z - 1))
            cot_part(v, dy * Z + 2, q, q, False).start()

    with scope("cot_on"):
        for dy in range(1, Y):
            cot_wait(dy * Z)
            q = frm(dy * Z)
            for dz in (1, Z - 1):
                for c in cots(dy * Z + dz, q, q):
                    c.start()
        for i in (1, Z - 1):
            cot_wait(i)
        cot_halves(0)
        for i in range(T):
            xfirst(i, t).start()

    with scope("stats_b"):
        for c in loc:
            c.wait()

        def sq_b(j, acc):
            v = kb[:, blk(j, DS)].astype(F32)
            return acc + jnp.sum(v * v, axis=-1, keepdims=True)

        total = lax.fori_loop(0, T, sq_b, jnp.zeros((R, 1), F32))
        inv_b[...] = jnp.broadcast_to(lax.rsqrt(total / D + EPS), (R, R))

    with scope("weff"):
        for i in range(1, T):
            for c in ups(i, frm(i)):
                c.wait_recv()
        WT = 256

        def weff(j, _):
            down = dnf[:, pl.ds(pl.multiple_of(t * DS + j * WT, WT), WT)]
            low = dot(down, upf[...], 0, 0)
            rows = blk(j, WT)
            wb[rows, :] = (wb[rows, :].astype(F32) + SCALE * low).astype(BF16)
            return 0

        lax.fori_loop(0, DS // WT, weff, 0)

    def x_on(dy):
        with scope("x_on"):
            for dz in range(1, Z):
                i = dy * Z + dz
                xfirst(i, frm(dy * Z)).wait_recv()
                xon(i, 0, frm(dy * Z)).start()

    with scope("wait_cot"):
        for dy in range(1, Y):
            for dz in (1, Z - 1):
                cot_wait(dy * Z + dz)
            cot_halves(dy)
        for dy in range(Y):
            cot_wait(dy * Z + 2)
    for i in range(1, T):
        for c in downs(i, t):
            c.start()
    for dy in range(Y):
        x_on(dy)
    rets().start()
    NT = 512

    def branch(p, store):
        c = cf[blk(p, R), :]
        for n in range(DS // NT):
            store(n, dot(c, wb[pl.ds(n * NT, NT), :], 1, 1).astype(BF16))

    def branch_to(i, _):
        p = to(i)

        def store(n, v):
            bro[p, :, pl.ds(n * NT, NT)] = v

        branch(p, store)
        return 0

    def store_own(n, v):
        bri[0, :, pl.ds(n * NT, NT)] = v

    with scope("branch"):
        lax.fori_loop(1, T, branch_to, 0)
        branch(t, store_own)

    def forward_block(i, r):
        invs(i).wait_recv()
        inv = jnp.broadcast_to(inv_i[i, 0:1, :], (R, R)).T
        normed = (
            xin[blk(r, R), :].astype(F32) * inv[:, 0:1] * gain[:, blk(t, DS)].astype(F32)
        ).astype(BF16)
        rows = blk(i, R)
        for n in range(2 * KV // NT):
            yo[rows, pl.ds(n * NT, NT)] = dot(normed, wb[:, pl.ds(n * NT, NT)], 1, 0).astype(BF16)

    def forward(i, _):
        forward_block(i, frm(i))
        return 0

    with scope("wait_x"):
        for i in range(T):
            if i % Z:
                send(xat.at[0], xin.at[blk(frm(i), R), :], XIN, i, (sec, to(i % Z))).wait_recv()
    for i in range(1, T):
        bras(i).start()

    with scope("forward"):
        for g in range(Y):
            xfirst(g * Z, frm(g * Z)).wait_recv()
            forward_block(g * Z, frm(g * Z))
            lax.fori_loop(g * Z + 1, (g + 1) * Z, forward, 0)
            for k in range(4):
                for c in parts(g, k):
                    c.start()

    with scope("kept"):
        for i in range(1, T):
            for c in downs(i, frm(i)):
                c.wait_recv()
        adapt = (SCALE * dot(upf[...], cf[blk(t, R), :], 1, 1)).astype(BF16)

        def kept_block(i, mid):
            p = to(i)
            cols = blk(p, DS)
            normed = (kb[:, cols].astype(F32) * inv_b[:, 0:1] * gain[:, cols].astype(F32)).astype(BF16)
            gdo[p] = dot(adapt, normed, 1, 0).astype(BF16)

            @pl.when(i > 0)
            def _():
                grds(i).start()

            return mid + dot(dnf[:, cols], normed, 1, 1)

        mid = lax.fori_loop(0, T, kept_block, jnp.zeros((2 * RK, R), F32))
        mid_o[...] = mid.astype(BF16)
        for i in range(1, T):
            mids(i).start()

    def rows_of(g, b, j):
        return blk(g * Z + lax.rem(z + 2 * Z - j - b, Z), R)

    def heads(v, hy, zz):
        return pl.ds(pl.multiple_of(v * KV + (hy * Z + zz) * H, H), H)

    for g in range(Y):
        with scope("wait_relay"):
            for k in range(2):
                for c in parts(g, k):
                    c.wait_recv()
        row = lax.rem(y + Y - g, Y)

        with scope("relay"):

            def pair_block(b, _):
                dst = blk(row * Z + b, R)
                for v in range(2):
                    zz = lax.rem(z + (1 if v == 0 else Z - 1), Z)
                    for w in range(Y):
                        acc = yo[rows_of(g, b, 0), heads(v, w, zz)].astype(F32)
                        acc = acc + yi[v, rows_of(g, b, 1 if v == 0 else Z - 1), pl.ds(w * H, H)].astype(F32)
                        yco[v, dst, pl.ds(w * H, H)] = acc.astype(BF16)
                return 0

            lax.fori_loop(0, Z, pair_block, 0)
            for v in range(2):
                pairs(g, v, row).start()

    with scope("wait_branch"):
        for i in range(1, T):
            bras(i).wait_recv()

    with scope("inner"):

        def inner_block(i, acc):
            cols = blk(frm(i), DS)
            scaled = gain[:, cols].astype(F32) * bri[i].astype(F32)
            return acc + jnp.sum(kb[:, cols].astype(F32) * scaled, axis=-1, keepdims=True)

        inner = lax.fori_loop(0, T, inner_block, jnp.zeros((R, 1), F32)) / D
    with scope("wait_ret"):
        rets().wait_recv()
    with scope("final"):
        inverse = inv_b[:, 0:1]
        factor = inverse * inverse * inverse * inner

        def final_block(i, _):
            cols = blk(frm(i), DS)
            scaled = gain[:, cols].astype(F32) * bri[i].astype(F32)
            back[:, cols] = (
                back[:, cols].astype(F32) + inverse * scaled - kb[:, cols].astype(F32) * factor
            ).astype(BF16)
            pltpu.make_async_copy(back.at[:, cols], igrad.at[:, cols], ols.at[i]).start()
            return 0

        lax.fori_loop(0, T, final_block, 0)

    for g in range(Y):
        with scope("wait_parts"):
            for k in (2, 3):
                for c in parts(g, k):
                    c.wait_recv()
            for v in range(2):
                pairs(g, v, lax.rem(y + Y - g, Y)).wait_recv()
        row = lax.rem(y + Y - g, Y)

        with scope("sum_parts"):

            def sum_block(b, _):
                dst = blk(row * Z + b, R)
                for w in range(Y):
                    hy = lax.rem(y + w, Y)
                    for v in range(2):
                        acc = yo[rows_of(g, b, 0), heads(v, hy, z)].astype(F32)
                        acc = acc + yi[2 + v, rows_of(g, b, Z - 1 if v == 0 else 1), blk(hy, H)].astype(F32)
                        acc = acc + yci[v, dst, blk(hy, H)].astype(F32)
                        if w == 0:
                            yt[dst, pl.ds(v * H, H)] = acc
                        else:
                            ys[w, dst, pl.ds(v * H, H)] = acc.astype(BF16)
                return 0

            lax.fori_loop(0, Z, sum_block, 0)
            for dy in range(1, Y):
                tots(g, dy, row).start()

    with scope("grads"):
        for i in range(1, T):
            grds(i).wait_recv()
            mids(i).wait_recv()
        g = gdo[t].astype(F32)
        for i in range(1, T):
            g = g + gdi[i].astype(F32)
        gkt[...] = g[0:RK]
        gvt[...] = g[RK : 2 * RK]

        def up_grad(i, acc):
            m = mid_i[i]
            rows = blk(frm(i), R)
            k = dot(m[0:RK], cf[rows, blk(t, H)], 1, 0)
            v = dot(m[RK : 2 * RK], cf[rows, vblk(t)], 1, 0)
            return acc[0] + k, acc[1] + v

        mid_i[0] = mid_o[...]
        k, v = lax.fori_loop(0, T, up_grad, (jnp.zeros((RK, H), F32), jnp.zeros((RK, H), F32)))
        guk[...] = SCALE * k
        guv[...] = SCALE * v

    with scope("wait_tot"):
        for g in range(Y):
            for dy in range(1, Y):
                tots(g, dy, lax.rem(y + 2 * Y - dy - g, Y)).wait_recv()

    def total_block(b, _):
        rows = blk(b, R)
        k = yt[rows, pl.ds(0, H)]
        v = yt[rows, pl.ds(H, H)]
        for dy in range(1, Y):
            k = k + yr[dy, rows, pl.ds(0, H)].astype(F32)
            v = v + yr[dy, rows, pl.ds(H, H)].astype(F32)
        keys[rows, :] = k.astype(BF16)
        vals[rows, :] = v.astype(BF16)
        return 0

    with scope("total"):
        lax.fori_loop(0, T, total_block, 0)

    with scope("end"):
        for i in range(1, T):
            for c in (*ups(i, t), *downs(i, t), bras(i), grds(i), mids(i)):
                c.wait_send()
        for i in range(1, T):
            for c in cots(i, t, t):
                c.wait_send()
        for g in range(Y):
            for k in range(4):
                for c in parts(g, k):
                    c.wait_send()
            for v in range(2):
                pairs(g, v, lax.rem(y + Y - g, Y)).wait_send()
            for dy in range(1, Y):
                tots(g, dy, lax.rem(y + Y - g, Y)).wait_send()
        for i in range(T):
            xfirst(i, t).wait_send()
            if i % Z:
                xon(i, 0, t).wait_send()
            invs(i).wait_send()
            cols = blk(frm(i), DS)
            pltpu.make_async_copy(back.at[:, cols], igrad.at[:, cols], ols.at[i]).wait()
        rets().wait_send()


def on_device(S, T, arr, kept, ret, gain, wk, wv, dk, dv, uk, uv, ck, cv):
    Y, Z = 2, T // 2
    _, R, D = arr.shape
    _, DS, KV = wk.shape
    RK, H = uk.shape[1:]
    any_ = pl.BlockSpec(memory_space=pl.ANY)
    vmem = pl.BlockSpec(memory_space=pltpu.VMEM)
    outs = pl.pallas_call(
        functools.partial(kernel, S, Y, Z),
        out_shape=(
            jax.ShapeDtypeStruct((R * T, H), BF16),
            jax.ShapeDtypeStruct((R * T, H), BF16),
            jax.ShapeDtypeStruct((R, D), BF16),
            jax.ShapeDtypeStruct((RK, DS), F32),
            jax.ShapeDtypeStruct((RK, DS), F32),
            jax.ShapeDtypeStruct((RK, H), F32),
            jax.ShapeDtypeStruct((RK, H), F32),
        ),
        in_specs=[any_, any_, any_, vmem] + [any_] * 8,
        out_specs=(vmem, vmem, any_, vmem, vmem, vmem, vmem),
        scratch_shapes=[
            pltpu.VMEM((DS, 2 * KV), BF16),
            pltpu.VMEM((R * T, 2 * KV), BF16),
            pltpu.VMEM((R * T, DS), BF16),
            pltpu.VMEM((Y * (Z - 1), R, DS), BF16),
            pltpu.VMEM((R, D), BF16),
            pltpu.VMEM((R, D), BF16),
            pltpu.VMEM((T, R, DS), BF16),
            pltpu.VMEM((T, R, DS), BF16),
            pltpu.VMEM((R * T, 2 * KV), BF16),
            pltpu.VMEM((4, R * T, Y * H), BF16),
            pltpu.VMEM((2, R * T, Y * H), BF16),
            pltpu.VMEM((2, R * T, Y * H), BF16),
            pltpu.VMEM((R * T, 2 * H), F32),
            pltpu.VMEM((Y, R * T, 2 * H), BF16),
            pltpu.VMEM((Y, R * T, 2 * H), BF16),
            pltpu.VMEM((2 * RK, D), BF16),
            pltpu.VMEM((T, 2 * RK, DS), BF16),
            pltpu.VMEM((T, 2 * RK, DS), BF16),
            pltpu.VMEM((2 * RK, 2 * KV), BF16),
            pltpu.VMEM((8, R), F32),
            pltpu.VMEM((T, 8, R), F32),
            pltpu.VMEM((2 * RK, R), BF16),
            pltpu.VMEM((T, 2 * RK, R), BF16),
            pltpu.VMEM((R, R), F32),
            pltpu.SemaphoreType.DMA((KINDS, T)),
            pltpu.SemaphoreType.DMA((KINDS, T)),
            pltpu.SemaphoreType.DMA((2, T)),
            pltpu.SemaphoreType.DMA((2, T)),
            pltpu.SemaphoreType.DMA((4 * Y * Y,)),
            pltpu.SemaphoreType.DMA((4 * Y * Y,)),
            pltpu.SemaphoreType.DMA((9 + T,)),
            pltpu.SemaphoreType.DMA((T,)),
        ],
        compiler_params=pltpu.CompilerParams(
            collective_id=0, has_side_effects=True, vmem_limit_bytes=62 * 2**20
        ),
    )(
        arr[0], kept[0], ret[0], gain, wk[0], wv[0], dk[0].T, dv[0].T, uk[0], uv[0], ck[0], cv[0]
    )
    keys, vals, igrad, gkt, gvt, guk, guv = outs
    return keys[None], vals[None], igrad[None], gkt.T[None], gvt.T[None], guk[None], guv[None]


def solution(mesh):
    S, T = mesh.shape["section"], mesh.shape["tensor"]
    return jax.shard_map(
        functools.partial(on_device, S, T),
        mesh=mesh,
        in_specs=(
            P("section", "tensor", None),
            P("section", "tensor", None),
            P("section", "tensor", None),
            P("section", None),
            P("section", "tensor", None),
            P("section", "tensor", None),
            P("section", "tensor", None),
            P("section", "tensor", None),
            P("section", None, "tensor"),
            P("section", None, "tensor"),
            P("section", None, "tensor"),
            P("section", None, "tensor"),
        ),
        out_specs=(
            P("section", None, "tensor"),
            P("section", None, "tensor"),
            P("section", "tensor", None),
            P("section", "tensor", None),
            P("section", "tensor", None),
            P("section", None, "tensor"),
            P("section", None, "tensor"),
        ),
        check_vma=False,
    )
```

```python
import contextlib
import functools

import jax
import jax.numpy as jnp
from jax import lax
from jax.experimental import pallas as pl
from jax.experimental.pallas import tpu as pltpu
from jax.sharding import PartitionSpec as P

EPS = 1e-05
SCALE = 2.0
F32 = jnp.float32
BF16 = jnp.bfloat16
MESH = pl.DeviceIdType.MESH

UPK, UPV, DNK, DNV, COTK, COTV, XAT, XIN, INV, RET, BRA, GRD, GRY, MID, PAR, TOT = range(16)
KINDS = 16


PROFILE = False


def scope(name):
    return jax.named_scope(name) if PROFILE else contextlib.nullcontext()


def dot(a, b, ca, cb):
    return lax.dot_general(a, b, (((ca,), (cb,)), ((), ())), preferred_element_type=F32)


def kernel(
    S, Y, Z,
    arr, kept, ret, gain, wk, wv, dkt, dvt, uk, uv, ck, cv,
    keys_h, vals_h, igrad, gkt_h, gvt_h, guk_h, guv_h,
    keys, vals, gkt, gvt, guk, guv,
    wb, cf, xin, xat, kb, back, bro, bri, yo, yi, yco, yci, yt, ys, yr, dnf, gdo, gdi, gds, gdr, upf,
    inv_o, inv_i, mid_o, mid_i, inv_b,
    ss, rs, yss, yrs, ls, ols,
):
    sec = lax.axis_index("section")
    t = lax.axis_index("tensor")
    T = Y * Z
    R = arr.shape[0]
    DS = wk.shape[0]
    H = ck.shape[1]
    KV = wk.shape[1]
    RK = uk.shape[0]
    D = T * DS
    nxt = lax.rem(sec + 1, S)
    prv = lax.rem(sec + S - 1, S)
    y = t // Z
    z = lax.rem(t, Z)

    def to(i):
        return lax.rem(y + i // Z, Y) * Z + lax.rem(z + lax.rem(i, Z), Z)

    def frm(i):
        return lax.rem(y + Y - i // Z, Y) * Z + lax.rem(z + Z - lax.rem(i, Z), Z)

    def blk(i, size):
        return pl.ds(pl.multiple_of(i * size, size), size)

    def vblk(i):
        return pl.ds(pl.multiple_of(KV + i * H, H), H)

    def remote(src, dst, ssem, rsem, device):
        return pltpu.make_async_remote_copy(
            src_ref=src, dst_ref=dst, send_sem=ssem, recv_sem=rsem,
            device_id=device, device_id_type=MESH,
        )

    def send(src, dst, kind, i, device):
        return remote(src, dst, ss.at[kind, i], rs.at[kind, i], device)

    def ups(i, r):
        dev = (sec, to(i))
        return (
            send(uk, upf.at[pl.ds(0, RK), blk(r, H)], UPK, i, dev),
            send(uv, upf.at[pl.ds(RK, RK), vblk(r)], UPV, i, dev),
        )

    def place(kind, v, b):
        if kind == COTK:
            return cf.at[:, blk(b, H) if v == 0 else vblk(b)]
        return dnf.at[pl.ds(v * RK, RK), blk(b, DS)]

    def spread_part(kind, v, i, q, r, own=False):
        dy, dz = i // Z, i % Z
        if dz == 2:
            dev = (sec, to(1 if v == 0 else Z - 1))
        else:
            dev = (sec, to(dz if dz else dy * Z))
        src = ((ck, cv) if kind == COTK else (dkt, dvt))[v] if own else place(kind, v, q)
        return send(src, place(kind, v, r), kind + v, i, dev)

    def spread(kind, i, q, r, own=False):
        return [spread_part(kind, v, i, q, r, own) for v in range(2)]

    def spread_own(kind):
        for dy in range(1, Y):
            for c in spread(kind, dy * Z, t, t, True):
                c.start()
        for i in (1, Z - 1):
            for c in spread(kind, i, t, t, True):
                c.start()

    def spread_wait(kind, i):
        for c in spread(kind, i, t, frm(i)):
            c.wait_recv()

    def spread_halves(kind, dy):
        for v in range(2):
            q = frm(dy * Z + (1 if v == 0 else Z - 1))
            spread_part(kind, v, dy * Z + 2, q, q).start()

    def spread_on(kind):
        for dy in range(1, Y):
            spread_wait(kind, dy * Z)
            q = frm(dy * Z)
            for dz in (1, Z - 1):
                for c in spread(kind, dy * Z + dz, q, q):
                    c.start()
        for i in (1, Z - 1):
            spread_wait(kind, i)
        spread_halves(kind, 0)

    def spread_on_2(kind):
        for dy in range(1, Y):
            for dz in (1, Z - 1):
                spread_wait(kind, dy * Z + dz)
            spread_halves(kind, dy)

    def spread_end(kind):
        for dy in range(Y):
            spread_wait(kind, dy * Z + 2)

    def xfirst(i, r):
        dy, dz = i // Z, i % Z
        cols = blk(lax.rem(y + dy, Y) * Z + lax.rem(z + dz, Z), DS)
        dst = xin.at[blk(r, R), :] if dz == 0 else xat.at[dy * (Z - 1) + dz - 1]
        return send(arr.at[:, cols], dst, XAT, i, (nxt, to(dy * Z)))

    def xon(i, q, r):
        dy, dz = i // Z, i % Z
        return send(xat.at[dy * (Z - 1) + dz - 1], xin.at[blk(r, R), :], XIN, i, (sec, to(dz)))

    def invs(i):
        return send(inv_o, inv_i.at[i], INV, i, (nxt, to(i)))

    def rets():
        return send(ret, back, RET, 0, (prv, t))

    def bras(i):
        return send(bro.at[to(i)], bri.at[i], BRA, i, (sec, to(i)))

    def grds(dz, w):
        zz = lax.rem(z + dz, Z)
        return send(gdo.at[w * Z + zz], gdi.at[dz * Y + w], GRD, dz * Y + w, (sec, to(dz)))

    def grys(dy):
        return send(gds.at[dy], gdr.at[dy], GRY, dy, (sec, to(dy * Z)))

    def mids(i):
        return send(mid_o, mid_i.at[i], MID, i, (sec, to(i)))

    RG = R * Z

    def parts(g, k):
        v = k % 2
        dz = (1, Z - 1, Z - 1, 1)[k]
        zz = lax.rem(z + (2 if k < 2 else dz), Z)
        out = []
        for w in range(Y):
            at = pl.multiple_of(v * KV + (w * Z + zz) * H, H)
            n = (g * 4 + k) * Y + w
            out.append(remote(
                yo.at[pl.ds(g * RG, RG), pl.ds(at, H)],
                yi.at[k, pl.ds(g * RG, RG), pl.ds(w * H, H)],
                yss.at[n], yrs.at[n], (sec, to(dz)),
            ))
        return out

    def pairs(g, v, row):
        return send(yco.at[v, blk(row, RG), :], yci.at[v, blk(row, RG), :], PAR, g * 2 + v, (sec, to(1 if v == 0 else Z - 1)))

    def tots(g, dy, row):
        return send(ys.at[dy, blk(row, RG), :], yr.at[dy, blk(row, RG), :], TOT, g * Y + dy, (sec, to(dy * Z)))

    bar = pltpu.get_barrier_semaphore()
    for i in range(1, T):
        pl.semaphore_signal(bar, inc=1, device_id=(sec, to(i)), device_id_type=MESH)
    for i in range(T):
        pl.semaphore_signal(bar, inc=1, device_id=(nxt, to(i)), device_id_type=MESH)
        pl.semaphore_signal(bar, inc=1, device_id=(prv, to(i)), device_id_type=MESH)

    arrs = [pltpu.make_async_copy(arr.at[:, pl.ds(j * DS, DS)], bro.at[j], ls.at[9 + j]) for j in range(T)]
    loc = [
        pltpu.make_async_copy(wk, wb.at[:, pl.ds(0, KV)], ls.at[0]),
        pltpu.make_async_copy(wv, wb.at[:, pl.ds(KV, KV)], ls.at[1]),
        pltpu.make_async_copy(uk, upf.at[pl.ds(0, RK), blk(t, H)], ls.at[2]),
        pltpu.make_async_copy(uv, upf.at[pl.ds(RK, RK), vblk(t)], ls.at[3]),
        pltpu.make_async_copy(dkt, dnf.at[pl.ds(0, RK), blk(t, DS)], ls.at[4]),
        pltpu.make_async_copy(dvt, dnf.at[pl.ds(RK, RK), blk(t, DS)], ls.at[5]),
        pltpu.make_async_copy(ck, cf.at[:, blk(t, H)], ls.at[6]),
        pltpu.make_async_copy(cv, cf.at[:, vblk(t)], ls.at[7]),
        pltpu.make_async_copy(kept, kb, ls.at[8]),
    ]
    for c in arrs:
        c.start()
    for c in loc:
        c.start()
    upf[pl.ds(0, RK), pl.ds(KV, KV)] = jnp.zeros((RK, KV), BF16)
    upf[pl.ds(RK, RK), pl.ds(0, KV)] = jnp.zeros((RK, KV), BF16)

    outs = [
        pltpu.make_async_copy(a, b, ols.at[T + n])
        for n, (a, b) in enumerate([(keys, keys_h), (vals, vals_h), (gkt, gkt_h), (gvt, gvt_h), (guk, guk_h), (guv, guv_h)])
    ]

    with scope("barrier"):
        pl.semaphore_wait(bar, 3 * T - 1)

    for i in range(1, T):
        for c in ups(i, t):
            c.start()
    spread_own(COTK)
    spread_own(DNK)

    with scope("stats_a"):
        for c in arrs:
            c.wait()

        def sq_a(j, acc):
            v = bro[j].astype(F32)
            return acc + jnp.sum(v * v, axis=-1, keepdims=True)

        total = lax.fori_loop(0, T, sq_a, jnp.zeros((R, 1), F32))
        inverse = lax.rsqrt(total / D + EPS)
        inv_o[...] = jnp.broadcast_to(inverse, (R, R)).T[0:8, :]
        for i in range(T):
            invs(i).start()

    with scope("cot_on"):
        spread_on(COTK)
        for i in range(T):
            xfirst(i, t).start()

    with scope("stats_b"):
        for c in loc:
            c.wait()

        def sq_b(j, acc):
            v = kb[:, blk(j, DS)].astype(F32)
            return acc + jnp.sum(v * v, axis=-1, keepdims=True)

        total = lax.fori_loop(0, T, sq_b, jnp.zeros((R, 1), F32))
        inv_b[...] = jnp.broadcast_to(lax.rsqrt(total / D + EPS), (R, R))

    with scope("weff"):
        for i in range(1, T):
            for c in ups(i, frm(i)):
                c.wait_recv()
        WT = 256

        def weff(j, _):
            down = dnf[:, pl.ds(pl.multiple_of(t * DS + j * WT, WT), WT)]
            low = dot(down, upf[...], 0, 0)
            rows = blk(j, WT)
            wb[rows, :] = (wb[rows, :].astype(F32) + SCALE * low).astype(BF16)
            return 0

        lax.fori_loop(0, DS // WT, weff, 0)

    def x_on(dy):
        with scope("x_on"):
            for dz in range(1, Z):
                i = dy * Z + dz
                xfirst(i, frm(dy * Z)).wait_recv()
                xon(i, 0, frm(dy * Z)).start()

    with scope("wait_cot"):
        spread_on(DNK)
        spread_on_2(COTK)
        spread_end(COTK)
    with scope("wait_down"):
        spread_on_2(DNK)
    x_on(0)
    NT = 512

    def branch(p, store):
        c = cf[blk(p, R), :]
        for n in range(DS // NT):
            store(n, dot(c, wb[pl.ds(n * NT, NT), :], 1, 1).astype(BF16))

    def branch_to(i, _):
        p = to(i)

        def store(n, v):
            bro[p, :, pl.ds(n * NT, NT)] = v

        branch(p, store)
        return 0

    def store_own(n, v):
        bri[0, :, pl.ds(n * NT, NT)] = v

    with scope("branch"):
        lax.fori_loop(Z, T, branch_to, 0)
    for dy in range(1, Y):
        x_on(dy)
    rets().start()
    with scope("branch"):
        lax.fori_loop(1, Z, branch_to, 0)
        branch(t, store_own)

    def forward_block(i, r):
        invs(i).wait_recv()
        inv = jnp.broadcast_to(inv_i[i, 0:1, :], (R, R)).T
        normed = (
            xin[blk(r, R), :].astype(F32) * inv[:, 0:1] * gain[:, blk(t, DS)].astype(F32)
        ).astype(BF16)
        rows = blk(i, R)
        for n in range(2 * KV // NT):
            yo[rows, pl.ds(n * NT, NT)] = dot(normed, wb[:, pl.ds(n * NT, NT)], 1, 0).astype(BF16)

    def forward(i, _):
        forward_block(i, frm(i))
        return 0

    def kept_normed(p):
        cols = blk(p, DS)
        return (kb[:, cols].astype(F32) * inv_b[:, 0:1] * gain[:, cols].astype(F32)).astype(BF16)

    with scope("kept"):
        adapt = (SCALE * dot(upf[...], cf[blk(t, R), :], 1, 1)).astype(BF16)

        def grad_block(p, _):
            gdo[p] = dot(adapt, kept_normed(p), 1, 0).astype(BF16)
            return 0

        lax.fori_loop(0, T, grad_block, 0)
    with scope("middle"):
        spread_end(DNK)

        def middle_block(p, mid):
            return mid + dot(dnf[:, blk(p, DS)], kept_normed(p), 1, 1)

        mid_o[...] = lax.fori_loop(0, T, middle_block, jnp.zeros((2 * RK, R), F32)).astype(BF16)
        for i in range(1, T):
            mids(i).start()

    with scope("wait_x"):
        for i in range(T):
            if i % Z:
                send(xat.at[0], xin.at[blk(frm(i), R), :], XIN, i, (sec, to(i % Z))).wait_recv()
    for i in range(Z, T):
        bras(i).start()
    for dz in range(1, Z):
        for w in range(Y):
            grds(dz, w).start()

    with scope("forward"):
        for g in range(Y):
            xfirst(g * Z, frm(g * Z)).wait_recv()
            forward_block(g * Z, frm(g * Z))
            lax.fori_loop(g * Z + 1, (g + 1) * Z, forward, 0)
            for k in range(4):
                for c in parts(g, k):
                    c.start()

    def rows_of(g, b, j):
        return blk(g * Z + lax.rem(z + 2 * Z - j - b, Z), R)

    def heads(v, hy, zz):
        return pl.ds(pl.multiple_of(v * KV + (hy * Z + zz) * H, H), H)

    for g in range(Y):
        with scope("wait_relay"):
            for k in range(2):
                for c in parts(g, k):
                    c.wait_recv()
        row = lax.rem(y + Y - g, Y)

        with scope("relay"):

            def pair_block(b, _):
                dst = blk(row * Z + b, R)
                for v in range(2):
                    zz = lax.rem(z + (1 if v == 0 else Z - 1), Z)
                    for w in range(Y):
                        acc = yo[rows_of(g, b, 0), heads(v, w, zz)].astype(F32)
                        acc = acc + yi[v, rows_of(g, b, 1 if v == 0 else Z - 1), pl.ds(w * H, H)].astype(F32)
                        yco[v, dst, pl.ds(w * H, H)] = acc.astype(BF16)
                return 0

            lax.fori_loop(0, Z, pair_block, 0)
            for v in range(2):
                pairs(g, v, row).start()

    for i in range(1, Z):
        bras(i).start()

    with scope("grads_z"):
        for dz in range(1, Z):
            for w in range(Y):
                grds(dz, w).wait_recv()

        def grad_sum(w):
            acc = gdo[w * Z + z].astype(F32)
            for dz in range(1, Z):
                acc = acc + gdi[dz * Y + w].astype(F32)
            return acc

        for dy in range(1, Y):
            gds[dy] = grad_sum(lax.rem(y + dy, Y)).astype(BF16)
            grys(dy).start()
        own_grad = grad_sum(y)
        gkt[...] = own_grad[0:RK]
        gvt[...] = own_grad[RK : 2 * RK]

    for g in range(Y):
        with scope("wait_parts"):
            for k in (2, 3):
                for c in parts(g, k):
                    c.wait_recv()
            for v in range(2):
                pairs(g, v, lax.rem(y + Y - g, Y)).wait_recv()
        row = lax.rem(y + Y - g, Y)

        with scope("sum_parts"):

            def sum_block(b, _):
                dst = blk(row * Z + b, R)
                for w in range(Y):
                    hy = lax.rem(y + w, Y)
                    for v in range(2):
                        acc = yo[rows_of(g, b, 0), heads(v, hy, z)].astype(F32)
                        acc = acc + yi[2 + v, rows_of(g, b, Z - 1 if v == 0 else 1), blk(hy, H)].astype(F32)
                        acc = acc + yci[v, dst, blk(hy, H)].astype(F32)
                        if w == 0:
                            yt[dst, pl.ds(v * H, H)] = acc
                        else:
                            ys[w, dst, pl.ds(v * H, H)] = acc.astype(BF16)
                return 0

            lax.fori_loop(0, Z, sum_block, 0)
            for dy in range(1, Y):
                tots(g, dy, row).start()

    with scope("grads"):
        for dy in range(1, Y):
            grys(dy).wait_recv()
            gkt[...] = gkt[...] + gdr[dy, 0:RK].astype(F32)
            gvt[...] = gvt[...] + gdr[dy, RK : 2 * RK].astype(F32)
        for i in range(1, T):
            mids(i).wait_recv()

        def up_grad(i, acc):
            m = mid_i[i]
            rows = blk(frm(i), R)
            k = dot(m[0:RK], cf[rows, blk(t, H)], 1, 0)
            v = dot(m[RK : 2 * RK], cf[rows, vblk(t)], 1, 0)
            return acc[0] + k, acc[1] + v

        mid_i[0] = mid_o[...]
        k, v = lax.fori_loop(0, T, up_grad, (jnp.zeros((RK, H), F32), jnp.zeros((RK, H), F32)))
        guk[...] = SCALE * k
        guv[...] = SCALE * v
        for c in outs[2:]:
            c.start()

    with scope("wait_tot"):
        for g in range(Y):
            for dy in range(1, Y):
                tots(g, dy, lax.rem(y + 2 * Y - dy - g, Y)).wait_recv()

    def total_block(b, _):
        rows = blk(b, R)
        k = yt[rows, pl.ds(0, H)]
        v = yt[rows, pl.ds(H, H)]
        for dy in range(1, Y):
            k = k + yr[dy, rows, pl.ds(0, H)].astype(F32)
            v = v + yr[dy, rows, pl.ds(H, H)].astype(F32)
        keys[rows, :] = k.astype(BF16)
        vals[rows, :] = v.astype(BF16)
        return 0

    with scope("total"):
        lax.fori_loop(0, T, total_block, 0)
        for c in outs[:2]:
            c.start()

    with scope("inner"):

        def inner_block(i, acc):
            cols = blk(frm(i), DS)
            scaled = gain[:, cols].astype(F32) * bri[i].astype(F32)
            return acc + jnp.sum(kb[:, cols].astype(F32) * scaled, axis=-1, keepdims=True)

        inner = inner_block(0, jnp.zeros((R, 1), F32))
        for i in (*range(Z, T), *range(1, Z)):
            bras(i).wait_recv()
            inner = inner_block(i, inner)
        inner = inner / D
    with scope("wait_ret"):
        rets().wait_recv()
    with scope("final"):
        inverse = inv_b[:, 0:1]
        factor = inverse * inverse * inverse * inner

        def final_block(i, _):
            cols = blk(frm(i), DS)
            scaled = gain[:, cols].astype(F32) * bri[i].astype(F32)
            back[:, cols] = (
                back[:, cols].astype(F32) + inverse * scaled - kb[:, cols].astype(F32) * factor
            ).astype(BF16)
            pltpu.make_async_copy(back.at[:, cols], igrad.at[:, cols], ols.at[i]).start()
            return 0

        lax.fori_loop(0, T, final_block, 0)

    with scope("end"):
        for i in range(1, T):
            for c in (*ups(i, t), *spread(COTK, i, t, t), *spread(DNK, i, t, t), bras(i), mids(i)):
                c.wait_send()
        for dz in range(1, Z):
            for w in range(Y):
                grds(dz, w).wait_send()
        for dy in range(1, Y):
            grys(dy).wait_send()
        for g in range(Y):
            for k in range(4):
                for c in parts(g, k):
                    c.wait_send()
            for v in range(2):
                pairs(g, v, lax.rem(y + Y - g, Y)).wait_send()
            for dy in range(1, Y):
                tots(g, dy, lax.rem(y + Y - g, Y)).wait_send()
        for i in range(T):
            xfirst(i, t).wait_send()
            if i % Z:
                xon(i, 0, t).wait_send()
            invs(i).wait_send()
            cols = blk(frm(i), DS)
            pltpu.make_async_copy(back.at[:, cols], igrad.at[:, cols], ols.at[i]).wait()
        rets().wait_send()
        for c in outs:
            c.wait()


def hand_on(cuts, *refs):
    n = len(cuts)
    src, dst, mid, (sem_in, sem_out) = refs[:n], refs[n : 2 * n], refs[2 * n : 3 * n], refs[3 * n :]
    ins, outs = [], []
    for a, b, m, cut in zip(src, dst, mid, cuts):
        rows = a.shape[0] // cut
        for c in range(cut):
            at = pl.ds(c * rows, rows)
            k = len(ins)
            ins.append(pltpu.make_async_copy(a.at[at], m.at[at], sem_in.at[k]))
            outs.append(pltpu.make_async_copy(m.at[at], b.at[at], sem_out.at[k]))
    for c in ins:
        c.start()
    for c, d in zip(ins, outs):
        c.wait()
        d.start()
    for d in outs:
        d.wait()


def on_device(S, T, arr, kept, ret, gain, wk, wv, dk, dv, uk, uv, ck, cv):
    Y, Z = 2, T // 2
    _, R, D = arr.shape
    _, DS, KV = wk.shape
    RK, H = uk.shape[1:]
    any_ = pl.BlockSpec(memory_space=pl.ANY)
    vmem = pl.BlockSpec(memory_space=pltpu.VMEM)
    outs = pl.pallas_call(
        functools.partial(kernel, S, Y, Z),
        out_shape=(
            jax.ShapeDtypeStruct((R * T, H), BF16),
            jax.ShapeDtypeStruct((R * T, H), BF16),
            jax.ShapeDtypeStruct((R, D), BF16),
            jax.ShapeDtypeStruct((RK, DS), F32),
            jax.ShapeDtypeStruct((RK, DS), F32),
            jax.ShapeDtypeStruct((RK, H), F32),
            jax.ShapeDtypeStruct((RK, H), F32),
        ),
        in_specs=[any_, any_, any_, vmem] + [any_] * 8,
        out_specs=(any_,) * 7,
        scratch_shapes=[
            pltpu.VMEM((R * T, H), BF16),
            pltpu.VMEM((R * T, H), BF16),
            pltpu.VMEM((RK, DS), F32),
            pltpu.VMEM((RK, DS), F32),
            pltpu.VMEM((RK, H), F32),
            pltpu.VMEM((RK, H), F32),
            pltpu.VMEM((DS, 2 * KV), BF16),
            pltpu.VMEM((R * T, 2 * KV), BF16),
            pltpu.VMEM((R * T, DS), BF16),
            pltpu.VMEM((Y * (Z - 1), R, DS), BF16),
            pltpu.VMEM((R, D), BF16),
            pltpu.VMEM((R, D), BF16),
            pltpu.VMEM((T, R, DS), BF16),
            pltpu.VMEM((T, R, DS), BF16),
            pltpu.VMEM((R * T, 2 * KV), BF16),
            pltpu.VMEM((4, R * T, Y * H), BF16),
            pltpu.VMEM((2, R * T, Y * H), BF16),
            pltpu.VMEM((2, R * T, Y * H), BF16),
            pltpu.VMEM((R * T, 2 * H), F32),
            pltpu.VMEM((Y, R * T, 2 * H), BF16),
            pltpu.VMEM((Y, R * T, 2 * H), BF16),
            pltpu.VMEM((2 * RK, D), BF16),
            pltpu.VMEM((T, 2 * RK, DS), BF16),
            pltpu.VMEM((T, 2 * RK, DS), BF16),
            pltpu.VMEM((Y, 2 * RK, DS), BF16),
            pltpu.VMEM((Y, 2 * RK, DS), BF16),
            pltpu.VMEM((2 * RK, 2 * KV), BF16),
            pltpu.VMEM((8, R), F32),
            pltpu.VMEM((T, 8, R), F32),
            pltpu.VMEM((2 * RK, R), BF16),
            pltpu.VMEM((T, 2 * RK, R), BF16),
            pltpu.VMEM((R, R), F32),
            pltpu.SemaphoreType.DMA((KINDS, T)),
            pltpu.SemaphoreType.DMA((KINDS, T)),
            pltpu.SemaphoreType.DMA((4 * Y * Y,)),
            pltpu.SemaphoreType.DMA((4 * Y * Y,)),
            pltpu.SemaphoreType.DMA((9 + T,)),
            pltpu.SemaphoreType.DMA((T + 6,)),
        ],
        compiler_params=pltpu.CompilerParams(
            collective_id=0, has_side_effects=True, vmem_limit_bytes=62 * 2**20
        ),
    )(
        arr[0], kept[0], ret[0], gain, wk[0], wv[0], dk[0].T, dv[0].T, uk[0], uv[0], ck[0], cv[0]
    )
    cuts = [1, 1, T, 1, 1, 1, 1]
    outs = pl.pallas_call(
        functools.partial(hand_on, cuts),
        out_shape=[jax.ShapeDtypeStruct(o.shape, o.dtype) for o in outs],
        in_specs=[any_] * 7,
        out_specs=[any_] * 7,
        scratch_shapes=[pltpu.VMEM(o.shape, o.dtype) for o in outs]
        + [pltpu.SemaphoreType.DMA((sum(cuts),)), pltpu.SemaphoreType.DMA((sum(cuts),))],
    )(*outs)
    keys, vals, igrad, gkt, gvt, guk, guv = outs
    return keys[None], vals[None], igrad[None], gkt.T[None], gvt.T[None], guk[None], guv[None]


def solution(mesh):
    S, T = mesh.shape["section"], mesh.shape["tensor"]
    return jax.shard_map(
        functools.partial(on_device, S, T),
        mesh=mesh,
        in_specs=(
            P("section", "tensor", None),
            P("section", "tensor", None),
            P("section", "tensor", None),
            P("section", None),
            P("section", "tensor", None),
            P("section", "tensor", None),
            P("section", "tensor", None),
            P("section", "tensor", None),
            P("section", None, "tensor"),
            P("section", None, "tensor"),
            P("section", None, "tensor"),
            P("section", None, "tensor"),
        ),
        out_specs=(
            P("section", None, "tensor"),
            P("section", None, "tensor"),
            P("section", "tensor", None),
            P("section", "tensor", None),
            P("section", "tensor", None),
            P("section", None, "tensor"),
            P("section", None, "tensor"),
        ),
        check_vma=False,
    )
```

```python
import contextlib
import functools

import jax
import jax.numpy as jnp
from jax import lax
from jax.experimental import pallas as pl
from jax.experimental.pallas import tpu as pltpu
from jax.sharding import PartitionSpec as P

EPS = 1e-05
SCALE = 2.0
F32 = jnp.float32
BF16 = jnp.bfloat16
MESH = pl.DeviceIdType.MESH

UPK, UPV, DNK, DNV, COTK, COTV, XAT, XIN, INV, RET, BRA, GRD, GRY, MID, PAR, TOT = range(16)


def slots(Y, Z):
    T = Y * Z
    first = [1, 1, 1, 1, 1, 1, 0, 1, 0, 0, 1, Y, 1, 1, 0, 1]
    count = [T - 1] * 6 + [T, T - 1, T, 1, T - 1, T - Y, Y - 1, T - 1, 2 * Y, 2 * Y - 1]
    at, base = 0, []
    for f, n in zip(first, count):
        base.append(at - f)
        at += n
    return base, at


PROFILE = False


def scope(name):
    return jax.named_scope(name) if PROFILE else contextlib.nullcontext()


def dot(a, b, ca, cb):
    return lax.dot_general(a, b, (((ca,), (cb,)), ((), ())), preferred_element_type=F32)


def kernel(
    S, Y, Z,
    arr, kept, ret, gain, wk, wv, dkt, dvt, uk, uv, ck, cv,
    keys_h, vals_h, igrad, gkt_h, gvt_h, guk_h, guv_h,
    keys, vals, gkt, gvt, guk, guv,
    wb, cf, xin, xat, kb, back, bro, bri, yo, yi, yco, yci, yt, ys, yr, dnf, gdo, gdi, gds, gdr, upf,
    inv_o, inv_i, mid_o, mid_i, inv_b,
    ss, rs, yss, yrs, ls, ols,
):
    sec = lax.axis_index("section")
    t = lax.axis_index("tensor")
    T = Y * Z
    R = arr.shape[0]
    DS = wk.shape[0]
    H = ck.shape[1]
    KV = wk.shape[1]
    RK = uk.shape[0]
    D = T * DS
    nxt = lax.rem(sec + 1, S)
    prv = lax.rem(sec + S - 1, S)
    base, _ = slots(Y, Z)
    y = t // Z
    z = lax.rem(t, Z)

    def to(i):
        return lax.rem(y + i // Z, Y) * Z + lax.rem(z + lax.rem(i, Z), Z)

    def frm(i):
        return lax.rem(y + Y - i // Z, Y) * Z + lax.rem(z + Z - lax.rem(i, Z), Z)

    def blk(i, size):
        return pl.ds(pl.multiple_of(i * size, size), size)

    def vblk(i):
        return pl.ds(pl.multiple_of(KV + i * H, H), H)

    def remote(src, dst, ssem, rsem, device):
        return pltpu.make_async_remote_copy(
            src_ref=src, dst_ref=dst, send_sem=ssem, recv_sem=rsem,
            device_id=device, device_id_type=MESH,
        )

    def send(src, dst, kind, i, device):
        return remote(src, dst, ss.at[base[kind] + i], rs.at[base[kind] + i], device)

    def ups(i, r):
        dev = (sec, to(i))
        return (
            send(uk, upf.at[pl.ds(0, RK), blk(r, H)], UPK, i, dev),
            send(uv, upf.at[pl.ds(RK, RK), vblk(r)], UPV, i, dev),
        )

    def place(kind, v, b):
        if kind == COTK:
            return cf.at[:, blk(b, H) if v == 0 else vblk(b)]
        return dnf.at[pl.ds(v * RK, RK), blk(b, DS)]

    def spread_part(kind, v, i, q, r, own=False):
        dy, dz = i // Z, i % Z
        if dz == 2:
            dev = (sec, to(1 if v == 0 else Z - 1))
        else:
            dev = (sec, to(dz if dz else dy * Z))
        src = ((ck, cv) if kind == COTK else (dkt, dvt))[v] if own else place(kind, v, q)
        return send(src, place(kind, v, r), kind + v, i, dev)

    def spread(kind, i, q, r, own=False):
        return [spread_part(kind, v, i, q, r, own) for v in range(2)]

    def spread_own(kind):
        for dy in range(1, Y):
            for c in spread(kind, dy * Z, t, t, True):
                c.start()
        for i in (1, Z - 1):
            for c in spread(kind, i, t, t, True):
                c.start()

    def spread_wait(kind, i):
        for c in spread(kind, i, t, frm(i)):
            c.wait_recv()

    def spread_halves(kind, dy):
        for v in range(2):
            q = frm(dy * Z + (1 if v == 0 else Z - 1))
            spread_part(kind, v, dy * Z + 2, q, q).start()

    def spread_on(kind):
        for dy in range(1, Y):
            spread_wait(kind, dy * Z)
            q = frm(dy * Z)
            for dz in (1, Z - 1):
                for c in spread(kind, dy * Z + dz, q, q):
                    c.start()
        for i in (1, Z - 1):
            spread_wait(kind, i)
        spread_halves(kind, 0)

    def spread_on_2(kind):
        for dy in range(1, Y):
            for dz in (1, Z - 1):
                spread_wait(kind, dy * Z + dz)
            spread_halves(kind, dy)

    def spread_end(kind):
        for dy in range(Y):
            spread_wait(kind, dy * Z + 2)

    def xfirst(i, r):
        dy, dz = i // Z, i % Z
        cols = blk(lax.rem(y + dy, Y) * Z + lax.rem(z + dz, Z), DS)
        dst = xin.at[blk(r, R), :] if dz == 0 else xat.at[dy * (Z - 1) + dz - 1]
        return send(arr.at[:, cols], dst, XAT, i, (nxt, to(dy * Z)))

    def xon(i, q, r):
        dy, dz = i // Z, i % Z
        return send(xat.at[dy * (Z - 1) + dz - 1], xin.at[blk(r, R), :], XIN, i, (sec, to(dz)))

    def invs(i):
        return send(inv_o, inv_i.at[i], INV, i, (nxt, to(i)))

    def rets():
        return send(ret, back, RET, 0, (prv, t))

    def bras(i):
        return send(bro.at[to(i)], bri.at[i], BRA, i, (sec, to(i)))

    def grds(dz, w):
        zz = lax.rem(z + dz, Z)
        return send(gdo.at[w * Z + zz], gdi.at[dz * Y + w], GRD, dz * Y + w, (sec, to(dz)))

    def grys(dy):
        return send(gds.at[dy], gdr.at[dy], GRY, dy, (sec, to(dy * Z)))

    def mids(i):
        return send(mid_o, mid_i.at[i], MID, i, (sec, to(i)))

    RG = R * Z

    def parts(g, k):
        v = k % 2
        dz = (1, Z - 1, Z - 1, 1)[k]
        zz = lax.rem(z + (2 if k < 2 else dz), Z)
        out = []
        for w in range(Y):
            at = pl.multiple_of(v * KV + (w * Z + zz) * H, H)
            n = (g * 4 + k) * Y + w
            out.append(remote(
                yo.at[pl.ds(g * RG, RG), pl.ds(at, H)],
                yi.at[k, pl.ds(g * RG, RG), pl.ds(w * H, H)],
                yss.at[n], yrs.at[n], (sec, to(dz)),
            ))
        return out

    def pairs(g, v, row):
        return send(yco.at[v, blk(row, RG), :], yci.at[v, blk(row, RG), :], PAR, g * 2 + v, (sec, to(1 if v == 0 else Z - 1)))

    def tots(g, dy, row):
        return send(ys.at[dy, blk(row, RG), :], yr.at[dy, blk(row, RG), :], TOT, g * Y + dy, (sec, to(dy * Z)))

    bar = pltpu.get_barrier_semaphore()
    for i in range(1, T):
        pl.semaphore_signal(bar, inc=1, device_id=(sec, to(i)), device_id_type=MESH)
    for i in range(T):
        pl.semaphore_signal(bar, inc=1, device_id=(nxt, to(i)), device_id_type=MESH)
        pl.semaphore_signal(bar, inc=1, device_id=(prv, to(i)), device_id_type=MESH)

    arrs = [pltpu.make_async_copy(arr.at[:, pl.ds(j * DS, DS)], bro.at[j], ls.at[9 + j]) for j in range(T)]
    loc = [
        pltpu.make_async_copy(wk, wb.at[:, pl.ds(0, KV)], ls.at[0]),
        pltpu.make_async_copy(wv, wb.at[:, pl.ds(KV, KV)], ls.at[1]),
        pltpu.make_async_copy(uk, upf.at[pl.ds(0, RK), blk(t, H)], ls.at[2]),
        pltpu.make_async_copy(uv, upf.at[pl.ds(RK, RK), vblk(t)], ls.at[3]),
        pltpu.make_async_copy(dkt, dnf.at[pl.ds(0, RK), blk(t, DS)], ls.at[4]),
        pltpu.make_async_copy(dvt, dnf.at[pl.ds(RK, RK), blk(t, DS)], ls.at[5]),
        pltpu.make_async_copy(ck, cf.at[:, blk(t, H)], ls.at[6]),
        pltpu.make_async_copy(cv, cf.at[:, vblk(t)], ls.at[7]),
        pltpu.make_async_copy(kept, kb, ls.at[8]),
    ]
    for c in arrs:
        c.start()
    for c in loc:
        c.start()
    upf[pl.ds(0, RK), pl.ds(KV, KV)] = jnp.zeros((RK, KV), BF16)
    upf[pl.ds(RK, RK), pl.ds(0, KV)] = jnp.zeros((RK, KV), BF16)

    outs = [
        pltpu.make_async_copy(a, b, ols.at[T + n])
        for n, (a, b) in enumerate([(keys, keys_h), (vals, vals_h), (gkt, gkt_h), (gvt, gvt_h), (guk, guk_h), (guv, guv_h)])
    ]

    with scope("barrier"):
        pl.semaphore_wait(bar, 3 * T - 1)

    for i in range(1, T):
        for c in ups(i, t):
            c.start()
    spread_own(COTK)
    spread_own(DNK)

    with scope("stats_a"):
        for c in arrs:
            c.wait()

        def sq_a(j, acc):
            v = bro[j].astype(F32)
            return acc + jnp.sum(v * v, axis=-1, keepdims=True)

        total = lax.fori_loop(0, T, sq_a, jnp.zeros((R, 1), F32))
        inverse = lax.rsqrt(total / D + EPS)
        inv_o[...] = jnp.broadcast_to(inverse, (R, R)).T[0:8, :]
        for i in range(T):
            invs(i).start()

    with scope("cot_on"):
        spread_on(COTK)
        for i in range(T):
            xfirst(i, t).start()

    with scope("stats_b"):
        for c in loc:
            c.wait()

        def sq_b(j, acc):
            v = kb[:, blk(j, DS)].astype(F32)
            return acc + jnp.sum(v * v, axis=-1, keepdims=True)

        total = lax.fori_loop(0, T, sq_b, jnp.zeros((R, 1), F32))
        inv_b[...] = jnp.broadcast_to(lax.rsqrt(total / D + EPS), (R, R))

    with scope("weff"):
        for i in range(1, T):
            for c in ups(i, frm(i)):
                c.wait_recv()
        WT = 256

        def weff(j, _):
            down = dnf[:, pl.ds(pl.multiple_of(t * DS + j * WT, WT), WT)]
            low = dot(down, upf[...], 0, 0)
            rows = blk(j, WT)
            wb[rows, :] = (wb[rows, :].astype(F32) + SCALE * low).astype(BF16)
            return 0

        lax.fori_loop(0, DS // WT, weff, 0)

    def x_on(dy):
        with scope("x_on"):
            for dz in range(1, Z):
                i = dy * Z + dz
                xfirst(i, frm(dy * Z)).wait_recv()
                xon(i, 0, frm(dy * Z)).start()

    with scope("wait_cot"):
        spread_on(DNK)
        spread_on_2(COTK)
    x_on(0)
    with scope("wait_down"):
        spread_on_2(DNK)
        spread_end(COTK)
    NT = 512

    def branch(p, store):
        c = cf[blk(p, R), :]
        for n in range(DS // NT):
            store(n, dot(c, wb[pl.ds(n * NT, NT), :], 1, 1).astype(BF16))

    def branch_to(i, _):
        p = to(i)

        def store(n, v):
            bro[p, :, pl.ds(n * NT, NT)] = v

        branch(p, store)
        return 0

    def store_own(n, v):
        bri[0, :, pl.ds(n * NT, NT)] = v

    with scope("branch"):
        lax.fori_loop(Z, T, branch_to, 0)
    for dy in range(1, Y):
        x_on(dy)
    rets().start()
    with scope("branch"):
        lax.fori_loop(1, Z, branch_to, 0)
        branch(t, store_own)

    def forward_block(i, r):
        invs(i).wait_recv()
        inv = jnp.broadcast_to(inv_i[i, 0:1, :], (R, R)).T
        normed = (
            xin[blk(r, R), :].astype(F32) * inv[:, 0:1] * gain[:, blk(t, DS)].astype(F32)
        ).astype(BF16)
        rows = blk(i, R)
        for n in range(2 * KV // NT):
            yo[rows, pl.ds(n * NT, NT)] = dot(normed, wb[:, pl.ds(n * NT, NT)], 1, 0).astype(BF16)

    def forward(i, _):
        forward_block(i, frm(i))
        return 0

    for i in range(Z, T):
        bras(i).start()

    def kept_normed(p):
        cols = blk(p, DS)
        return (kb[:, cols].astype(F32) * inv_b[:, 0:1] * gain[:, cols].astype(F32)).astype(BF16)

    with scope("kept"):
        adapt = (SCALE * dot(upf[...], cf[blk(t, R), :], 1, 1)).astype(BF16)

        def grad_block(p, _):
            gdo[p] = dot(adapt, kept_normed(p), 1, 0).astype(BF16)
            return 0

        lax.fori_loop(0, T, grad_block, 0)
    with scope("wait_x"):
        for i in range(T):
            if i % Z:
                send(xat.at[0], xin.at[blk(frm(i), R), :], XIN, i, (sec, to(i % Z))).wait_recv()
    for dz in range(1, Z):
        for w in range(Y):
            grds(dz, w).start()

    with scope("forward"):
        for g in range(Y):
            xfirst(g * Z, frm(g * Z)).wait_recv()
            forward_block(g * Z, frm(g * Z))
            lax.fori_loop(g * Z + 1, (g + 1) * Z, forward, 0)
            for k in range(4):
                for c in parts(g, k):
                    c.start()

    with scope("middle"):
        spread_end(DNK)

        def middle_block(p, mid):
            return mid + dot(dnf[:, blk(p, DS)], kept_normed(p), 1, 1)

        mid_o[...] = lax.fori_loop(0, T, middle_block, jnp.zeros((2 * RK, R), F32)).astype(BF16)
        for i in range(1, T):
            mids(i).start()

    def rows_of(g, b, j):
        return blk(g * Z + lax.rem(z + 2 * Z - j - b, Z), R)

    def heads(v, hy, zz):
        return pl.ds(pl.multiple_of(v * KV + (hy * Z + zz) * H, H), H)

    for g in range(Y):
        with scope("wait_relay"):
            for k in range(2):
                for c in parts(g, k):
                    c.wait_recv()
        row = lax.rem(y + Y - g, Y)

        with scope("relay"):

            def pair_block(b, _):
                dst = blk(row * Z + b, R)
                for v in range(2):
                    zz = lax.rem(z + (1 if v == 0 else Z - 1), Z)
                    for w in range(Y):
                        acc = yo[rows_of(g, b, 0), heads(v, w, zz)].astype(F32)
                        acc = acc + yi[v, rows_of(g, b, 1 if v == 0 else Z - 1), pl.ds(w * H, H)].astype(F32)
                        yco[v, dst, pl.ds(w * H, H)] = acc.astype(BF16)
                return 0

            lax.fori_loop(0, Z, pair_block, 0)
            for v in range(2):
                pairs(g, v, row).start()

    for i in range(1, Z):
        bras(i).start()

    with scope("grads_z"):
        for dz in range(1, Z):
            for w in range(Y):
                grds(dz, w).wait_recv()

        def grad_sum(w):
            acc = gdo[w * Z + z].astype(F32)
            for dz in range(1, Z):
                acc = acc + gdi[dz * Y + w].astype(F32)
            return acc

        for dy in range(1, Y):
            gds[dy] = grad_sum(lax.rem(y + dy, Y)).astype(BF16)
            grys(dy).start()
        own_grad = grad_sum(y)
        gkt[...] = own_grad[0:RK]
        gvt[...] = own_grad[RK : 2 * RK]

    for g in range(Y):
        with scope("wait_parts"):
            for k in (2, 3):
                for c in parts(g, k):
                    c.wait_recv()
            for v in range(2):
                pairs(g, v, lax.rem(y + Y - g, Y)).wait_recv()
        row = lax.rem(y + Y - g, Y)

        with scope("sum_parts"):

            def sum_block(b, _):
                dst = blk(row * Z + b, R)
                for w in range(Y):
                    hy = lax.rem(y + w, Y)
                    for v in range(2):
                        acc = yo[rows_of(g, b, 0), heads(v, hy, z)].astype(F32)
                        acc = acc + yi[2 + v, rows_of(g, b, Z - 1 if v == 0 else 1), blk(hy, H)].astype(F32)
                        acc = acc + yci[v, dst, blk(hy, H)].astype(F32)
                        if w == 0:
                            yt[dst, pl.ds(v * H, H)] = acc
                        else:
                            ys[w, dst, pl.ds(v * H, H)] = acc.astype(BF16)
                return 0

            lax.fori_loop(0, Z, sum_block, 0)
            for dy in range(1, Y):
                tots(g, dy, row).start()

    with scope("grads"):
        for dy in range(1, Y):
            grys(dy).wait_recv()
            gkt[...] = gkt[...] + gdr[dy, 0:RK].astype(F32)
            gvt[...] = gvt[...] + gdr[dy, RK : 2 * RK].astype(F32)
        for i in range(1, T):
            mids(i).wait_recv()

        def up_grad(i, acc):
            m = mid_i[i]
            rows = blk(frm(i), R)
            k = dot(m[0:RK], cf[rows, blk(t, H)], 1, 0)
            v = dot(m[RK : 2 * RK], cf[rows, vblk(t)], 1, 0)
            return acc[0] + k, acc[1] + v

        mid_i[0] = mid_o[...]
        k, v = lax.fori_loop(0, T, up_grad, (jnp.zeros((RK, H), F32), jnp.zeros((RK, H), F32)))
        guk[...] = SCALE * k
        guv[...] = SCALE * v
        for c in outs[2:]:
            c.start()

    with scope("inner"):

        def inner_block(i, acc):
            cols = blk(frm(i), DS)
            scaled = gain[:, cols].astype(F32) * bri[i].astype(F32)
            return acc + jnp.sum(kb[:, cols].astype(F32) * scaled, axis=-1, keepdims=True)

        inner = inner_block(0, jnp.zeros((R, 1), F32))
        for i in range(Z, T):
            bras(i).wait_recv()
            inner = inner_block(i, inner)

    with scope("wait_tot"):
        for g in range(Y):
            for dy in range(1, Y):
                tots(g, dy, lax.rem(y + 2 * Y - dy - g, Y)).wait_recv()

    def total_block(b, _):
        rows = blk(b, R)
        k = yt[rows, pl.ds(0, H)]
        v = yt[rows, pl.ds(H, H)]
        for dy in range(1, Y):
            k = k + yr[dy, rows, pl.ds(0, H)].astype(F32)
            v = v + yr[dy, rows, pl.ds(H, H)].astype(F32)
        keys[rows, :] = k.astype(BF16)
        vals[rows, :] = v.astype(BF16)
        return 0

    with scope("total"):
        lax.fori_loop(0, T, total_block, 0)
        for c in outs[:2]:
            c.start()

    with scope("inner_2"):
        for i in range(1, Z):
            bras(i).wait_recv()
            inner = inner_block(i, inner)
        inner = inner / D
    with scope("wait_ret"):
        rets().wait_recv()
    with scope("final"):
        inverse = inv_b[:, 0:1]
        factor = inverse * inverse * inverse * inner

        def final_block(i, _):
            cols = blk(frm(i), DS)
            scaled = gain[:, cols].astype(F32) * bri[i].astype(F32)
            back[:, cols] = (
                back[:, cols].astype(F32) + inverse * scaled - kb[:, cols].astype(F32) * factor
            ).astype(BF16)
            pltpu.make_async_copy(back.at[:, cols], igrad.at[:, cols], ols.at[i]).start()
            return 0

        lax.fori_loop(0, T, final_block, 0)

    with scope("end"):
        for i in range(1, T):
            for c in (*ups(i, t), *spread(COTK, i, t, t), *spread(DNK, i, t, t), bras(i), mids(i)):
                c.wait_send()
        for dz in range(1, Z):
            for w in range(Y):
                grds(dz, w).wait_send()
        for dy in range(1, Y):
            grys(dy).wait_send()
        for g in range(Y):
            for k in range(4):
                for c in parts(g, k):
                    c.wait_send()
            for v in range(2):
                pairs(g, v, lax.rem(y + Y - g, Y)).wait_send()
            for dy in range(1, Y):
                tots(g, dy, lax.rem(y + Y - g, Y)).wait_send()
        for i in range(T):
            xfirst(i, t).wait_send()
            if i % Z:
                xon(i, 0, t).wait_send()
            invs(i).wait_send()
            cols = blk(frm(i), DS)
            pltpu.make_async_copy(back.at[:, cols], igrad.at[:, cols], ols.at[i]).wait()
        rets().wait_send()
        for c in outs:
            c.wait()


def hand_on(cuts, *refs):
    n = len(cuts)
    src, dst, mid, (sem_in, sem_out) = refs[:n], refs[n : 2 * n], refs[2 * n : 3 * n], refs[3 * n :]
    ins, outs = [], []
    for a, b, m, cut in zip(src, dst, mid, cuts):
        rows = a.shape[0] // cut
        for c in range(cut):
            at = pl.ds(c * rows, rows)
            k = len(ins)
            ins.append(pltpu.make_async_copy(a.at[at], m.at[at], sem_in.at[k]))
            outs.append(pltpu.make_async_copy(m.at[at], b.at[at], sem_out.at[k]))
    for c in ins:
        c.start()
    for c, d in zip(ins, outs):
        c.wait()
        d.start()
    for d in outs:
        d.wait()


def on_device(S, T, arr, kept, ret, gain, wk, wv, dk, dv, uk, uv, ck, cv):
    Y, Z = 2, T // 2
    _, R, D = arr.shape
    _, DS, KV = wk.shape
    RK, H = uk.shape[1:]
    any_ = pl.BlockSpec(memory_space=pl.ANY)
    vmem = pl.BlockSpec(memory_space=pltpu.VMEM)
    outs = pl.pallas_call(
        functools.partial(kernel, S, Y, Z),
        out_shape=(
            jax.ShapeDtypeStruct((R * T, H), BF16),
            jax.ShapeDtypeStruct((R * T, H), BF16),
            jax.ShapeDtypeStruct((R, D), BF16),
            jax.ShapeDtypeStruct((RK, DS), F32),
            jax.ShapeDtypeStruct((RK, DS), F32),
            jax.ShapeDtypeStruct((RK, H), F32),
            jax.ShapeDtypeStruct((RK, H), F32),
        ),
        in_specs=[any_, any_, any_, vmem] + [any_] * 8,
        out_specs=(any_,) * 7,
        scratch_shapes=[
            pltpu.VMEM((R * T, H), BF16),
            pltpu.VMEM((R * T, H), BF16),
            pltpu.VMEM((RK, DS), F32),
            pltpu.VMEM((RK, DS), F32),
            pltpu.VMEM((RK, H), F32),
            pltpu.VMEM((RK, H), F32),
            pltpu.VMEM((DS, 2 * KV), BF16),
            pltpu.VMEM((R * T, 2 * KV), BF16),
            pltpu.VMEM((R * T, DS), BF16),
            pltpu.VMEM((Y * (Z - 1), R, DS), BF16),
            pltpu.VMEM((R, D), BF16),
            pltpu.VMEM((R, D), BF16),
            pltpu.VMEM((T, R, DS), BF16),
            pltpu.VMEM((T, R, DS), BF16),
            pltpu.VMEM((R * T, 2 * KV), BF16),
            pltpu.VMEM((4, R * T, Y * H), BF16),
            pltpu.VMEM((2, R * T, Y * H), BF16),
            pltpu.VMEM((2, R * T, Y * H), BF16),
            pltpu.VMEM((R * T, 2 * H), F32),
            pltpu.VMEM((Y, R * T, 2 * H), BF16),
            pltpu.VMEM((Y, R * T, 2 * H), BF16),
            pltpu.VMEM((2 * RK, D), BF16),
            pltpu.VMEM((T, 2 * RK, DS), BF16),
            pltpu.VMEM((T, 2 * RK, DS), BF16),
            pltpu.VMEM((Y, 2 * RK, DS), BF16),
            pltpu.VMEM((Y, 2 * RK, DS), BF16),
            pltpu.VMEM((2 * RK, 2 * KV), BF16),
            pltpu.VMEM((8, R), F32),
            pltpu.VMEM((T, 8, R), F32),
            pltpu.VMEM((2 * RK, R), BF16),
            pltpu.VMEM((T, 2 * RK, R), BF16),
            pltpu.VMEM((R, R), F32),
            pltpu.SemaphoreType.DMA((slots(Y, Z)[1],)),
            pltpu.SemaphoreType.DMA((slots(Y, Z)[1],)),
            pltpu.SemaphoreType.DMA((4 * Y * Y,)),
            pltpu.SemaphoreType.DMA((4 * Y * Y,)),
            pltpu.SemaphoreType.DMA((9 + T,)),
            pltpu.SemaphoreType.DMA((T + 6,)),
        ],
        compiler_params=pltpu.CompilerParams(
            collective_id=0, has_side_effects=True, vmem_limit_bytes=62 * 2**20
        ),
    )(
        arr[0], kept[0], ret[0], gain, wk[0], wv[0], dk[0].T, dv[0].T, uk[0], uv[0], ck[0], cv[0]
    )
    cuts = [1, 1, T, 1, 1, 1, 1]
    outs = pl.pallas_call(
        functools.partial(hand_on, cuts),
        out_shape=[jax.ShapeDtypeStruct(o.shape, o.dtype) for o in outs],
        in_specs=[any_] * 7,
        out_specs=[any_] * 7,
        scratch_shapes=[pltpu.VMEM(o.shape, o.dtype) for o in outs]
        + [pltpu.SemaphoreType.DMA((sum(cuts),)), pltpu.SemaphoreType.DMA((sum(cuts),))],
    )(*outs)
    keys, vals, igrad, gkt, gvt, guk, guv = outs
    return keys[None], vals[None], igrad[None], gkt.T[None], gvt.T[None], guk[None], guv[None]


def solution(mesh):
    S, T = mesh.shape["section"], mesh.shape["tensor"]
    return jax.shard_map(
        functools.partial(on_device, S, T),
        mesh=mesh,
        in_specs=(
            P("section", "tensor", None),
            P("section", "tensor", None),
            P("section", "tensor", None),
            P("section", None),
            P("section", "tensor", None),
            P("section", "tensor", None),
            P("section", "tensor", None),
            P("section", "tensor", None),
            P("section", None, "tensor"),
            P("section", None, "tensor"),
            P("section", None, "tensor"),
            P("section", None, "tensor"),
        ),
        out_specs=(
            P("section", None, "tensor"),
            P("section", None, "tensor"),
            P("section", "tensor", None),
            P("section", "tensor", None),
            P("section", "tensor", None),
            P("section", None, "tensor"),
            P("section", None, "tensor"),
        ),
        check_vma=False,
    )
```
